128 devices in a mesh: lat: 8 (over x, core), lon: 16 (over z, y).
Axes of the slice: x: 4, y: 4, z: 4, core: 2. Of those that a mesh axis runs over, the one named last changes fastest.
Arguments:
- grid_latent: bfloat16 [32, 2048, 512], P('lat', 'lon'), may hold values from -6 to 6
- mesh_latent: bfloat16 [16384, 512], P(('lat', 'lon')), may hold values from -6 to 6
- g2m_edges: bfloat16 [262144, 512], P(('lat', 'lon')), may hold values from -6 to 6
- g2m_senders: int32 [128, 2048], P(('lat', 'lon')), may hold values from 0 to 1631, as said below
- g2m_receivers: int32 [128, 2048], P(('lat', 'lon')), may hold values from 0 to 127, as said below
- mm_edges: bfloat16 [262144, 512], P(('lat', 'lon')), may hold values from -6 to 6
- mm_senders: int32 [128, 2048], P(('lat', 'lon')), may hold values from 0 to 2175
- mm_receivers: int32 [128, 2048], P(('lat', 'lon')), may hold values from 0 to 128, as said below
- send_rows: int32 [128, 2048], P(('lat', 'lon')), may hold values from 0 to 127
- edge_in: bfloat16 [3, 3, 512, 512], replicated, may hold values from -0.15625 to 0.15625
- edge_out: bfloat16 [3, 512, 512], replicated, may hold values from -0.25 to 0.25
- node_in: bfloat16 [3, 2, 512, 512], replicated, may hold values from -0.1875 to 0.1875
- node_out: bfloat16 [3, 512, 512], replicated, may hold values from -0.25 to 0.25
- norm_gain: float32 [3, 2, 512], replicated, may hold values from 0.5 to 1.5
- norm_bias: float32 [3, 2, 512], replicated, may hold values from -1.5 to 1.5
Outputs:
- mesh_out: bfloat16 [16384, 512], P(('lat', 'lon'))
The draws below stay inside these ranges and needn't reach their ends.
Inputs may be any that keep to these rules, and one draw needn't show every extreme that they name: `g2m_receivers`: each patch's edges are sorted by receiver; every mesh node of a patch receives at least one grid-to-mesh edge; the sender cell lies within 4 rows and columns of a cell that is fixed for the receiving node. `g2m_senders`: A flat index into the tile extended by 4 cells, with rows of 136 cells. `mm_receivers`: sorted within a patch; the used slots come first and the unused ones hold 128; some patch uses all 2048 slots in every draw.
All inputs are finite; a program needn't handle non-finite values.
Results may differ from the reference program's by a relative error of at most 0.012.
Values may be sent and summed in bfloat16 or wider, within the bound.
No kernel may reach another device: no remote copies, remote signals or barrier semaphores. Data moves between devices by JAX's collectives and lax.ppermute only.
A program may use at most 128 MiB of HBM per device.

```python
import jax
import jax.numpy as jnp
from jax import lax

LATENT = 512
GLAT = 4
GLON = 128
HALO = 4
MESH_DEV = 128
G2M_DEV = 2048
MM_DEV = 2048
CAP = 16
LAYERS = 2
BLOCKS = 3
NLAT = 32
NLON = 2048
MESH = 16384
N_LON = 16
DEVICES = 128


def node_spots(key):
    spot_rows = jax.random.randint(jax.random.fold_in(key, 11), (DEVICES, MESH_DEV), 0, GLAT)
    spot_cols = jax.random.randint(jax.random.fold_in(key, 12), (DEVICES, MESH_DEV), 0, GLON)
    return (spot_rows, spot_cols)


def draw_g2m_receivers(key, part):
    every_node = jnp.broadcast_to(jnp.arange(MESH_DEV, dtype=jnp.int32), (DEVICES, MESH_DEV))
    extra = jax.random.randint(jax.random.fold_in(key, 21), (DEVICES, G2M_DEV - MESH_DEV), 0, MESH_DEV)
    return jnp.sort(jnp.concatenate([every_node, extra.astype(jnp.int32)], axis=1), axis=1).astype(jnp.int32)


def draw_g2m_senders(key, part):
    receivers = draw_g2m_receivers(key, part)
    spot_rows, spot_cols = node_spots(key)
    row_steps = jax.random.randint(jax.random.fold_in(key, 31), (DEVICES, G2M_DEV), 0, 2 * HALO + 1)
    col_steps = jax.random.randint(jax.random.fold_in(key, 32), (DEVICES, G2M_DEV), 0, 2 * HALO + 1)
    cell_rows = jnp.take_along_axis(spot_rows, receivers, axis=1) + row_steps
    cell_cols = jnp.take_along_axis(spot_cols, receivers, axis=1) + col_steps
    return (cell_rows * (GLON + 2 * HALO) + cell_cols).astype(jnp.int32)


def draw_mm_receivers(key, part):
    counts = jax.random.randint(jax.random.fold_in(key, 41), (DEVICES,), MM_DEV // 3, MM_DEV + 1)
    filled = jax.random.randint(jax.random.fold_in(key, 42), (), 0, DEVICES)
    counts = jnp.where(jnp.arange(DEVICES, dtype=jnp.int32) == filled, MM_DEV, counts)
    drawn = jnp.sort(jax.random.randint(jax.random.fold_in(key, 43), (DEVICES, MM_DEV), 0, MESH_DEV), axis=1)
    places = jnp.arange(MM_DEV, dtype=jnp.int32)
    return jnp.where(places[None, :] < counts[:, None], drawn, MESH_DEV).astype(jnp.int32)


def draw_mm_senders(key, part):
    living = draw_mm_receivers(key, part) < MESH_DEV
    branch_pick = jax.random.randint(jax.random.fold_in(key, 51), (DEVICES, MM_DEV), 0, 4)
    faraway = jnp.logical_and(living, branch_pick > 0)
    ranks = jnp.cumsum(faraway.astype(jnp.int32), axis=1) - 1
    slot_total = DEVICES * CAP
    patch_keys = jax.random.split(jax.random.fold_in(key, 53), DEVICES)
    orders = jax.vmap(lambda one_key: jax.random.permutation(one_key, slot_total))(patch_keys).astype(jnp.int32)
    positions = (jnp.maximum(ranks, 0) % slot_total).astype(jnp.int32)
    remote = MESH_DEV + jnp.take_along_axis(orders, positions, axis=1)
    nearby = jax.random.randint(jax.random.fold_in(key, 52), (DEVICES, MM_DEV), 0, MESH_DEV)
    return jnp.where(faraway, remote, nearby).astype(jnp.int32)


def plant(values, own_key, least, high):
    longest = values.shape.index(max(values.shape))
    spots = []
    for shift in (0, 1):
        where = [jax.random.randint(jax.random.fold_in(own_key, axis), (), 0, length) for axis, length in enumerate(values.shape)]
        where[longest] = (where[longest] + shift) % values.shape[longest]
        spots.append(tuple(where))
    return values.at[spots[0]].set(least).at[spots[1]].set(high)


def block_levels(own_key, dims, cuts, low, top_value):
    level, own = 1.0, jax.random.fold_in(own_key, 6)
    for axis_at, parts in cuts:
        heights = jnp.exp(jax.random.uniform(jax.random.fold_in(own, axis_at), (parts,), jnp.float32, low / len(cuts), top_value / len(cuts)))
        level = level * jnp.repeat(heights, dims[axis_at] // parts).reshape([-1 if axis == axis_at else 1 for axis in range(len(dims))])
    return level


def scatter_about(stream_key, dims, scale, limit, pieces=(), kind=jnp.bfloat16):
    values = jax.random.normal(stream_key, dims, jnp.float32) * scale
    if len(pieces) > 0:
        values = block_levels(stream_key, dims, pieces, -0.22, 0.18) * values
    return jnp.clip(values, min=-limit, max=limit).astype(kind)


def setup_inputs(seed: int = 0) -> dict:
    key_of = jax.random.split(jax.random.key(seed), 16)
    return {
        "grid_latent": scatter_about(key_of[0], (NLAT, NLON, LATENT), 1.0, 6.0, ((0, 8), (1, 16))),
        "mesh_latent": scatter_about(key_of[1], (MESH, LATENT), 1.0, 6.0, ((0, 128),)),
        "g2m_edges": scatter_about(key_of[2], (DEVICES * G2M_DEV, LATENT), 1.0, 6.0, ((0, 128),)),
        "g2m_senders": draw_g2m_senders(jax.random.fold_in(key_of[15], 71), 0),
        "g2m_receivers": draw_g2m_receivers(jax.random.fold_in(key_of[15], 71), 0),
        "mm_edges": scatter_about(key_of[5], (DEVICES * MM_DEV, LATENT), 1.0, 6.0, ((0, 128),)),
        "mm_senders": draw_mm_senders(jax.random.fold_in(key_of[15], 71), 0),
        "mm_receivers": draw_mm_receivers(jax.random.fold_in(key_of[15], 71), 0),
        "send_rows": plant(jax.random.randint(key_of[8], (DEVICES, DEVICES * CAP), 0, MESH_DEV), jax.random.fold_in(key_of[8], 1), 0, MESH_DEV - 1).astype(jnp.int32),
        "edge_in": scatter_about(key_of[9], (BLOCKS, 3, LATENT, LATENT), (3 * LATENT) ** -0.5, 0.15625),
        "edge_out": scatter_about(key_of[10], (BLOCKS, LATENT, LATENT), LATENT ** -0.5, 0.25),
        "node_in": scatter_about(key_of[11], (BLOCKS, 2, LATENT, LATENT), (2 * LATENT) ** -0.5, 0.1875),
        "node_out": scatter_about(key_of[12], (BLOCKS, LATENT, LATENT), LATENT ** -0.5, 0.25),
        "norm_gain": jnp.clip(1.0 + 0.1 * jax.random.normal(key_of[13], (BLOCKS, 2, LATENT), jnp.float32), 0.5, 1.5),
        "norm_bias": scatter_about(key_of[14], (BLOCKS, 2, LATENT), 0.3, 1.5, (), jnp.float32),
    }


NORM_EPS = 1e-05

def normalize(values, gains, biases):
    centre = lax.optimization_barrier(jnp.mean(values, axis=-1, keepdims=True))
    spread = lax.optimization_barrier(jnp.mean(jnp.square(values - centre), axis=-1, keepdims=True))
    return (values - centre) * lax.rsqrt(spread + NORM_EPS) * gains + biases

def project(values, weights):
    return jnp.dot(values, weights, preferred_element_type=jnp.float32).astype(jnp.bfloat16)

def edge_update(edge_rows, sender_terms, receiver_terms, weights_in, weights_out, gains, biases):
    pre_act = jnp.dot(edge_rows, weights_in, preferred_element_type=jnp.float32)
    pre_act = pre_act + sender_terms.astype(jnp.float32) + receiver_terms.astype(jnp.float32)
    hidden = jax.nn.silu(pre_act).astype(jnp.bfloat16)
    output = jnp.dot(hidden, weights_out, preferred_element_type=jnp.float32)
    return (edge_rows.astype(jnp.float32) + normalize(output, gains, biases)).astype(jnp.bfloat16)

def node_update(nodes, summed, weights_in, weights_out, gains, biases):
    pre_act = jnp.dot(nodes, weights_in[0], preferred_element_type=jnp.float32)
    pre_act = pre_act + jnp.dot(summed.astype(jnp.bfloat16), weights_in[1], preferred_element_type=jnp.float32)
    hidden = jax.nn.silu(pre_act).astype(jnp.bfloat16)
    output = jnp.dot(hidden, weights_out, preferred_element_type=jnp.float32)
    return (nodes.astype(jnp.float32) + normalize(output, gains, biases)).astype(jnp.bfloat16)

def reference(grid_latent, mesh_latent, g2m_edges, g2m_senders, g2m_receivers, mm_edges, mm_senders, mm_receivers, send_rows, edge_in, edge_out, node_in, node_out, norm_gain, norm_bias):
    device_ids = jnp.arange(DEVICES, dtype=jnp.int32)
    grid_terms = project(grid_latent.reshape(-1, LATENT), edge_in[0, 1]).reshape(NLAT, NLON, LATENT)
    wrapped = jnp.concatenate([grid_terms[:, NLON - HALO:], grid_terms, grid_terms[:, :HALO]], axis=1)
    padded = jnp.pad(wrapped, ((HALO, HALO), (0, 0), (0, 0)))
    lookup = padded.reshape(-1, LATENT)
    tile_width = GLON + 2 * HALO
    lat_ids = device_ids // N_LON
    lon_ids = device_ids % N_LON
    glob_rows = lat_ids[:, None] * GLAT + g2m_senders // tile_width
    glob_cols = lon_ids[:, None] * GLON + g2m_senders % tile_width
    glob_send = (glob_rows * (NLON + 2 * HALO) + glob_cols).astype(jnp.int32)
    receiver_table = project(mesh_latent, edge_in[0, 2])

    def encode_device(items):
        edge_rows, senders, receivers, device = items
        sent = jnp.take(lookup, senders, axis=0)
        got = jnp.take(receiver_table, device * MESH_DEV + receivers, axis=0)
        updated = edge_update(edge_rows, sent, got, edge_in[0, 0], edge_out[0], norm_gain[0, 0], norm_bias[0, 0])
        return jax.ops.segment_sum(updated.astype(jnp.float32), receivers, num_segments=MESH_DEV)
    summed = lax.map(encode_device, (g2m_edges.reshape(DEVICES, G2M_DEV, LATENT), glob_send, g2m_receivers, device_ids))
    mesh_nodes = node_update(mesh_latent, summed.reshape(-1, LATENT), node_in[0], node_out[0], norm_gain[0, 1], norm_bias[0, 1])
    sources = send_rows.reshape(DEVICES, DEVICES, CAP) + (device_ids * MESH_DEV)[:, None, None]
    remote_index = jnp.transpose(sources, (1, 0, 2)).reshape(DEVICES, DEVICES * CAP).astype(jnp.int32)
    nearby = mm_senders < MESH_DEV
    far_index = jnp.take_along_axis(remote_index, jnp.clip(mm_senders - MESH_DEV, 0, DEVICES * CAP - 1).astype(jnp.int32), axis=1)
    glob_mm = jnp.where(nearby, device_ids[:, None] * MESH_DEV + mm_senders, far_index).astype(jnp.int32)
    alive = mm_receivers < MESH_DEV
    local_recv = jnp.minimum(mm_receivers, MESH_DEV - 1).astype(jnp.int32)
    edge_state = mm_edges.reshape(DEVICES, MM_DEV, LATENT)
    for level in range(1, LAYERS + 1):
        sender_table = project(mesh_nodes, edge_in[level, 1])
        recv_table = project(mesh_nodes, edge_in[level, 2])

        def process_device(items):
            edge_rows, senders, receivers, living, device = items
            sent = jnp.take(sender_table, senders, axis=0)
            got = jnp.take(recv_table, device * MESH_DEV + receivers, axis=0)
            updated = edge_update(edge_rows, sent, got, edge_in[level, 0], edge_out[level], norm_gain[level, 0], norm_bias[level, 0])
            kept = jnp.where(living[:, None], updated.astype(jnp.float32), jnp.float32(0.0))
            return (updated, jax.ops.segment_sum(kept, receivers, num_segments=MESH_DEV))
        edge_state, summed = lax.map(process_device, (edge_state, glob_mm, local_recv, alive, device_ids))
        mesh_nodes = node_update(mesh_nodes, summed.reshape(-1, LATENT), node_in[level], node_out[level], norm_gain[level, 1], norm_bias[level, 1])
    return mesh_nodes
```

```python
import functools

import jax
import jax.numpy as jnp
from jax import lax
from jax.experimental import pallas as pl
from jax.experimental.pallas import tpu as pltpu
from jax.sharding import PartitionSpec as P

HALO = 4
NORM_EPS = 1e-05
F32 = jnp.float32
BF16 = jnp.bfloat16
BLOCK = 256
GROUP = 16
MIB = 1024 * 1024


def silu(values):
    half = values * 0.5
    return half + half * jnp.tanh(half)


def normalize(values, gains, biases):
    centre = jnp.mean(values, axis=-1, keepdims=True)
    shifted = values - centre
    spread = jnp.mean(shifted * shifted, axis=-1, keepdims=True)
    return shifted * lax.rsqrt(spread + NORM_EPS) * gains + biases


def dot(left, right):
    return jnp.dot(left, right, preferred_element_type=F32)


def project(values, weights):
    return dot(values, weights).astype(BF16)


def hot_columns(indices, nodes):
    places = lax.broadcasted_iota(jnp.int32, (nodes, indices.shape[1]), 0)
    return jnp.where(places == indices, 1.0, 0.0).astype(BF16)


def hot_rows(indices, nodes):
    places = lax.broadcasted_iota(jnp.int32, (nodes, indices.shape[1]), 0)
    return jnp.where(places == indices, 1.0, 0.0).T.astype(BF16)


def pre_kernel(extra, edges, receivers, nodes, w_edge, w_recv, *refs):
    if extra:
        tile, w_send, send_rows, pre, tile_terms, picks = refs
    else:
        (pre,) = refs
    node_count = nodes.shape[0]
    terms = project(nodes[...], w_recv[...])
    edge_count = edges.shape[0]

    def step(i, _):
        at = pl.multiple_of(i * BLOCK, BLOCK)
        rows = pl.ds(at, BLOCK)
        hot = hot_rows(jnp.minimum(receivers[:, rows], node_count - 1), node_count)
        pre[rows, :] = dot(edges[rows, :], w_edge[...]) + dot(hot, terms)
        if extra:
            picks[rows, :] = hot_rows(send_rows[:, rows], node_count)
        return 0

    lax.fori_loop(0, edge_count // BLOCK, step, 0)
    if extra:
        tile_terms[...] = project(tile[...], w_send[...])


def main_kernel(pieces, last, keep, senders, receivers, pre, edges, w_out, edge_norm, nodes,
                w_node, w_node_out, node_norm, *refs):
    refs = list(refs)
    tables = [refs.pop(0) for _ in range(pieces)]
    w_send = refs.pop(0) if pieces > 2 else None
    if not last:
        w_next, picks = refs.pop(0), refs.pop(0)
    new_nodes = refs.pop(0)
    if not last:
        outgoing, out_rows = refs.pop(0), refs.pop(0)
    new_edges = refs.pop(0) if keep else None
    table, hidden, total = refs
    node_count = nodes.shape[0]
    edge_count = edges.shape[0]

    start = 0
    for index, piece in enumerate(tables):
        size = piece.shape[0]
        if w_send is not None and index > 0:
            values = project(piece[...], w_send[...]).astype(F32)
        else:
            values = piece[...].astype(F32)
        table[start:start + size, :] = values
        start += size

    total[...] = jnp.zeros_like(total)
    sublane = lax.broadcasted_iota(jnp.int32, (8, table.shape[1]), 0)

    def step(i, _):
        at = pl.multiple_of(i * BLOCK, BLOCK)
        rows = pl.ds(at, BLOCK)
        for group in range(BLOCK // GROUP):
            parts = []
            for half in range(GROUP // 8):
                first = group * GROUP + half * 8
                gathered = None
                for j in range(8):
                    row = senders[at + (first + j)]
                    value = jnp.broadcast_to(table[pl.ds(row, 1), :], sublane.shape)
                    gathered = value if j == 0 else jnp.where(sublane == j, value, gathered)
                begin = pl.multiple_of(at + first, 8)
                parts.append(silu(pre[pl.ds(begin, 8), :] + gathered))
            hidden[group * GROUP:(group + 1) * GROUP, :] = jnp.concatenate(parts, 0).astype(BF16)
        output = dot(hidden[...], w_out[...])
        fresh = edges[rows, :].astype(F32) + normalize(output, edge_norm[0:1, :], edge_norm[1:2, :])
        fresh = fresh.astype(BF16)
        if keep:
            new_edges[rows, :] = fresh
        total[...] += dot(hot_columns(receivers[:, rows], node_count), fresh)
        return 0

    lax.fori_loop(0, edge_count // BLOCK, step, 0)

    here = nodes[...]
    pre_node = dot(here, w_node[0]) + dot(total[...].astype(BF16), w_node[1])
    output = dot(silu(pre_node).astype(BF16), w_node_out[...])
    updated = here.astype(F32) + normalize(output, node_norm[0:1, :], node_norm[1:2, :])
    updated = updated.astype(BF16)
    new_nodes[...] = updated
    if not last:
        sent = project(updated, w_next[...])
        outgoing[...] = sent

        def pick(i, _):
            rows = pl.ds(pl.multiple_of(i * BLOCK, BLOCK), BLOCK)
            out_rows[rows, :] = dot(picks[rows, :], sent).astype(BF16)
            return 0

        lax.fori_loop(0, picks.shape[0] // BLOCK, pick, 0)


VMEM = pl.BlockSpec(memory_space=pltpu.VMEM)
SMEM = pl.BlockSpec(memory_space=pltpu.SMEM)


def pre_stage(edges, receivers, nodes, w_edge, w_recv, extra=()):
    edge_count, width = edges.shape
    node_count = nodes.shape[0]
    out_shape = [jax.ShapeDtypeStruct((edge_count, width), F32)]
    if extra:
        out_shape += [
            jax.ShapeDtypeStruct(extra[0].shape, BF16),
            jax.ShapeDtypeStruct((extra[2].shape[1], node_count), BF16),
        ]
    operands = (edges, receivers, nodes, w_edge, w_recv, *extra)
    return pl.pallas_call(
        functools.partial(pre_kernel, bool(extra)),
        out_shape=out_shape,
        in_specs=[VMEM] * len(operands),
        out_specs=[VMEM] * len(out_shape),
        name="pre_first" if extra else "pre_next",
        cost_estimate=pl.CostEstimate(
            flops=2 * edge_count * width * (width + node_count),
            bytes_accessed=edge_count * width * 6,
            transcendentals=0,
        ),
        compiler_params=pltpu.CompilerParams(vmem_limit_bytes=24 * MIB),
    )(*operands)


def main_stage(senders, receivers, pre, edges, w_out, edge_norm, nodes, w_node, w_node_out,
               node_norm, tables, w_send, following, keep, name):
    edge_count, width = edges.shape
    node_count = nodes.shape[0]
    operands = [senders, receivers, pre, edges, w_out, edge_norm, nodes, w_node, w_node_out,
                node_norm, *tables]
    if w_send is not None:
        operands.append(w_send)
    out_shape = []
    out_shape.append(jax.ShapeDtypeStruct((node_count, width), BF16))
    if following is not None:
        operands += list(following)
        out_shape.append(jax.ShapeDtypeStruct((node_count, width), BF16))
        out_shape.append(jax.ShapeDtypeStruct((following[1].shape[0], width), BF16))
    if keep:
        out_shape.append(jax.ShapeDtypeStruct((edge_count, width), BF16))
    table_rows = sum(piece.shape[0] for piece in tables)
    return pl.pallas_call(
        functools.partial(main_kernel, len(tables), following is None, keep),
        out_shape=out_shape,
        in_specs=[SMEM] + [VMEM] * (len(operands) - 1),
        out_specs=[VMEM] * len(out_shape),
        scratch_shapes=[
            pltpu.VMEM((table_rows, width), F32),
            pltpu.VMEM((BLOCK, width), BF16),
            pltpu.VMEM((node_count, width), F32),
        ],
        name=name,
        cost_estimate=pl.CostEstimate(
            flops=2 * edge_count * width * (width + node_count),
            bytes_accessed=edge_count * width * 10,
            transcendentals=edge_count * width,
        ),
        compiler_params=pltpu.CompilerParams(vmem_limit_bytes=32 * MIB),
    )(*operands)


def shift(array, axis, step, wrap):
    size = lax.axis_size(axis)
    pairs = [(i, (i + step) % size) for i in range(size) if wrap or 0 <= i + step < size]
    return lax.ppermute(array, axis, pairs)


def local(
    grid_latent,
    mesh_latent,
    g2m_edges,
    g2m_senders,
    g2m_receivers,
    mm_edges,
    mm_senders,
    mm_receivers,
    send_rows,
    edge_in,
    edge_out,
    node_in,
    node_out,
    norm_gain,
    norm_bias,
):
    high, wide, features = grid_latent.shape
    norms = jnp.stack([norm_gain, norm_bias], axis=2)

    west = shift(grid_latent[:, wide - HALO:, :], "lon", 1, True)
    east = shift(grid_latent[:, :HALO, :], "lon", -1, True)
    north = shift(grid_latent, "lat", 1, False)
    south = shift(grid_latent, "lat", -1, False)
    sides = jnp.concatenate([west, east], axis=1)
    north_sides = shift(sides, "lat", 1, False)
    south_sides = shift(sides, "lat", -1, False)

    tile_width = wide + 2 * HALO
    cell = g2m_senders[0]
    row, column = cell // tile_width, cell % tile_width
    band = jnp.where(row < HALO, 1, jnp.where(row < HALO + high, 0, 2))
    inner = row - jnp.where(band == 1, 0, jnp.where(band == 0, HALO, HALO + high))
    tile_cells = high * wide
    side_width = 2 * HALO
    side = jnp.where(column < HALO, column, column - wide)
    inside = jnp.logical_and(column >= HALO, column < HALO + wide)
    places = jnp.where(
        inside,
        band * tile_cells + inner * wide + column - HALO,
        3 * tile_cells + (band * high + inner) * side_width + side,
    )

    flat_tile = grid_latent.reshape(tile_cells, features)
    pre, tile_terms, picks = pre_stage(
        g2m_edges, g2m_receivers, mesh_latent, edge_in[0, 0], edge_in[0, 2],
        (flat_tile, edge_in[0, 1], send_rows),
    )
    all_sides = jnp.concatenate([sides, north_sides, south_sides], axis=0)
    tables = [
        tile_terms,
        north.reshape(tile_cells, features),
        south.reshape(tile_cells, features),
        all_sides.reshape(-1, features),
    ]
    nodes, outgoing, out_rows = main_stage(
        places, g2m_receivers, pre, g2m_edges, edge_out[0], norms[0, 0], mesh_latent, node_in[0],
        node_out[0], norms[0, 1], tables, edge_in[0, 1], (edge_in[1, 1], picks), False, "encode",
    )
    edges = mm_edges
    levels = edge_in.shape[0]
    for level in range(1, levels):
        devices = lax.axis_size("lat") * lax.axis_size("lon")
        blocks = out_rows.reshape(devices, -1, features)
        arrived = lax.all_to_all(blocks, ("lat", "lon"), split_axis=0, concat_axis=0, tiled=True)
        arrived = arrived.reshape(-1, features)
        (pre,) = pre_stage(edges, mm_receivers, nodes, edge_in[level, 0], edge_in[level, 2])
        final = level == levels - 1
        following = None if final else (edge_in[level + 1, 1], picks)
        results = main_stage(
            mm_senders[0], mm_receivers, pre, edges, edge_out[level], norms[level, 0], nodes,
            node_in[level], node_out[level], norms[level, 1], [outgoing, arrived], None, following,
            not final, "layer",
        )
        if final:
            (nodes,) = results
        else:
            nodes, outgoing, out_rows, edges = results
    return nodes


def solution(mesh):
    in_specs = (
        P("lat", "lon", None),
        P(("lat", "lon"), None),
        P(("lat", "lon"), None),
        P(("lat", "lon"), None),
        P(("lat", "lon"), None),
        P(("lat", "lon"), None),
        P(("lat", "lon"), None),
        P(("lat", "lon"), None),
        P(("lat", "lon"), None),
        P(),
        P(),
        P(),
        P(),
        P(),
        P(),
    )
    out_specs = P(("lat", "lon"), None)
    return jax.shard_map(local, mesh=mesh, in_specs=in_specs, out_specs=out_specs, check_vma=False)
```

```python
import functools

import jax
import jax.numpy as jnp
from jax import lax
from jax.experimental import pallas as pl
from jax.experimental.pallas import tpu as pltpu
from jax.sharding import PartitionSpec as P

HALO = 4
NORM_EPS = 1e-05
F32 = jnp.float32
BF16 = jnp.bfloat16
I32 = jnp.int32
BLOCK = 256
CHUNK = 256
LANES = 128
MIB = 1024 * 1024


def silu(values):
    half = values * 0.5
    return half + half * jnp.tanh(half)


def normalize(values, gains, biases):
    centre = jnp.mean(values, axis=-1, keepdims=True)
    shifted = values - centre
    spread = jnp.mean(shifted * shifted, axis=-1, keepdims=True)
    return shifted * lax.rsqrt(spread + NORM_EPS) * gains + biases


def dot(left, right):
    return jnp.dot(left, right, preferred_element_type=F32)


def project(values, weights):
    return dot(values, weights).astype(BF16)


def hot_columns(indices, nodes):
    places = lax.broadcasted_iota(I32, (nodes, indices.shape[1]), 0)
    return jnp.where(places == indices, 1.0, 0.0)


def hot_rows(indices, nodes):
    return hot_columns(indices, nodes).T.astype(BF16)


def line_of(row, tiles):
    return (row >> 3) * (8 * tiles) + (row & 7)


def cell_row(cell, high, wide):
    across = wide + 2 * HALO
    row = (cell * 241) >> 15
    column = cell - row * across
    band = jnp.where(row < HALO, 1, jnp.where(row < HALO + high, 0, 2))
    inner = row - jnp.where(band == 1, 0, jnp.where(band == 0, HALO, HALO + high))
    cells = high * wide
    tall = (high + 2 * HALO) * HALO
    side = 3 * cells + row * HALO
    west = side + column
    east = side + tall + column - HALO - wide
    centre = band * cells + inner * wide + column - HALO
    return jnp.where(column < HALO, west, jnp.where(column < HALO + wide, centre, east))


def begin(source, target, sem):
    copy = pltpu.make_async_copy(source, target, sem)
    copy.start()
    return copy


def part(ref, i):
    return ref.at[pl.ds(pl.multiple_of(i * BLOCK, BLOCK), BLOCK)]


def pre_kernel(level, shape, edges_h, receivers_h, nodes_h, edge_in_h, *refs):
    refs = list(refs)
    take = lambda count: [refs.pop(0) for _ in range(count)]
    if shape:
        tile_h, send_rows_h, cells_h, senders_h = take(4)
    pre_h = take(1)[0]
    if shape:
        tile_terms_h, picks_h, places_h, lines_h = take(4)
    edges, receivers, nodes, w_edge, w_recv, pre = take(6)
    if shape:
        tile, w_send, send_rows, cells, senders, tile_terms, picks, places, lines = take(9)
    sems, edge_sems, out_sems = take(3)
    node_count = nodes.shape[0]
    blocks = edges.shape[0] // BLOCK

    def edge_copy(i):
        return pltpu.make_async_copy(part(edges_h, i), part(edges, i), edge_sems.at[i])

    def out_copy(i):
        return pltpu.make_async_copy(part(pre, i), part(pre_h, i), out_sems.at[i])

    first = [
        begin(nodes_h, nodes, sems.at[0]),
        begin(edge_in_h.at[level, 2], w_recv, sems.at[1]),
        begin(receivers_h, receivers, sems.at[2]),
        begin(edge_in_h.at[level, 0], w_edge, sems.at[3]),
    ]
    for i in range(blocks):
        edge_copy(i).start()
    if shape:
        second = [
            begin(tile_h, tile, sems.at[4]),
            begin(edge_in_h.at[level, 1], w_send, sems.at[5]),
            begin(send_rows_h, send_rows, sems.at[6]),
            begin(cells_h, cells, sems.at[7]),
            begin(senders_h, senders, sems.at[8]),
        ]
    for copy in first:
        copy.wait()
    terms = project(nodes[...], w_recv[...])

    def step(i, _):
        rows = pl.ds(pl.multiple_of(i * BLOCK, BLOCK), BLOCK)
        edge_copy(i).wait()
        hot = hot_rows(jnp.minimum(receivers[:, rows], node_count - 1), node_count)
        pre[rows, :] = dot(edges[rows, :], w_edge[...]) + dot(hot, terms)
        out_copy(i).start()
        return 0

    lax.fori_loop(0, blocks, step, 0)
    if shape:
        high, wide = shape
        tiles = edges.shape[1] // LANES
        for copy in second:
            copy.wait()
        tile_terms[...] = project(tile[...], w_send[...])
        ends = [begin(tile_terms, tile_terms_h, sems.at[9])]

        def pick(i, _):
            rows = pl.ds(pl.multiple_of(i * BLOCK, BLOCK), BLOCK)
            picks[rows, :] = hot_rows(send_rows[:, rows], node_count)
            return 0

        lax.fori_loop(0, picks.shape[0] // BLOCK, pick, 0)
        ends.append(begin(picks, picks_h, sems.at[10]))
        places[...] = line_of(cell_row(cells[...], high, wide), tiles)
        lines[...] = line_of(senders[...], tiles)
        ends.append(begin(places, places_h, sems.at[11]))
        ends.append(begin(lines, lines_h, sems.at[12]))
    for i in range(blocks):
        out_copy(i).wait()
    if shape:
        for copy in ends:
            copy.wait()


def fill_table(table, start, values):
    tiles = values.shape[1] // LANES
    for group in range(values.shape[0] // 8):
        for tile in range(tiles):
            line = pl.multiple_of(start * tiles + (group * tiles + tile) * 8, 8)
            table[pl.ds(line, 8), :] = values[group * 8:group * 8 + 8, tile * LANES:(tile + 1) * LANES]


def main_kernel(level, pieces, last, keep, *refs):
    refs = list(refs)
    take = lambda count: [refs.pop(0) for _ in range(count)]
    places_h, receivers_h, pre_h, edges_h, nodes_h = take(5)
    edge_in_h, edge_out_h, node_in_h, node_out_h, gain_h, bias_h = take(6)
    sources = take(pieces)
    picks_h = None if last else take(1)[0]
    new_nodes_h = take(1)[0]
    outgoing_h, out_rows_h = (None, None) if last else take(2)
    new_edges_h = take(1)[0] if keep else None
    table, hidden_0, hidden_1, total, places, receivers, pre, edges = take(8)
    nodes, w_out, w_node, w_node_out, gain, bias, new_nodes, local_rows = take(8)
    w_send = take(1)[0] if pieces > 2 else None
    w_next, picks, outgoing, out_rows = (None,) * 4 if last else take(4)
    fresh_edges = take(1)[0] if keep else None
    sems, pre_sems, edge_sems, out_sems = take(4)

    node_count, width = nodes.shape
    blocks = edges.shape[0] // BLOCK
    tiles = width // LANES

    def pre_copy(i):
        return pltpu.make_async_copy(part(pre_h, i), part(pre, i), pre_sems.at[i])

    def edge_copy(i):
        return pltpu.make_async_copy(part(edges_h, i), part(edges, i), edge_sems.at[i])

    def fresh_copy(i):
        return pltpu.make_async_copy(part(fresh_edges, i), part(new_edges_h, i), out_sems.at[i])

    local_copy = begin(sources[0], local_rows, sems.at[0])
    places_copy = begin(places_h, places, sems.at[1])
    if w_send is not None:
        send_copy = begin(edge_in_h.at[level, 1], w_send, sems.at[2])
    pre_copy(0).start()
    second = [
        begin(edge_out_h.at[level], w_out, sems.at[3]),
        begin(receivers_h, receivers, sems.at[4]),
        begin(gain_h, gain, sems.at[5]),
        begin(bias_h, bias, sems.at[6]),
    ]
    edge_copy(0).start()
    for i in range(1, blocks):
        pre_copy(i).start()
        edge_copy(i).start()
    third = [
        begin(nodes_h, nodes, sems.at[7]),
        begin(node_in_h.at[level], w_node, sems.at[8]),
        begin(node_out_h.at[level], w_node_out, sems.at[9]),
    ]
    if not last:
        third.append(begin(edge_in_h.at[level + 1, 1], w_next, sems.at[10]))
        third.append(begin(picks_h, picks, sems.at[11]))

    total[...] = jnp.zeros_like(total)
    start = local_rows.shape[0]
    if w_send is not None:
        send_copy.wait()
    for source in sources[1:]:
        size = source.shape[0]
        for at in range(0, size, min(size, CHUNK)):
            values = source[at:at + min(size, CHUNK), :]
            if w_send is not None:
                values = project(values, w_send[...])
            fill_table(table, start + at, values.astype(F32))
        start += size
    local_copy.wait()
    fill_table(table, 0, local_rows[...].astype(F32))
    places_copy.wait()

    sublane = lax.broadcasted_iota(I32, (8, LANES), 0)
    chosen = [sublane == j for j in range(8)]

    def found(at):
        lines = [places[0, at + j] for j in range(8)]
        result = []
        for tile in range(tiles):
            value = None
            for j in range(8):
                row = jnp.broadcast_to(table[pl.ds(lines[j] + 8 * tile, 1), :], (8, LANES))
                value = row if j == 0 else jnp.where(chosen[j], row, value)
            result.append(value)
        return result

    def gather(i, hidden):
        at = pl.multiple_of(i * BLOCK, BLOCK)
        for group in range(BLOCK // 16):
            halves = []
            for half in range(2):
                offset = group * 16 + half * 8
                rows = found(at + offset)
                lead = pl.ds(pl.multiple_of(at + offset, 8), 8)
                halves.append([
                    silu(pre[lead, t * LANES:(t + 1) * LANES] + rows[t]) for t in range(tiles)
                ])
            for t in range(tiles):
                both = jnp.concatenate([halves[0][t], halves[1][t]], axis=0).astype(BF16)
                hidden[group * 16:group * 16 + 16, t * LANES:(t + 1) * LANES] = both

    def update(i, hidden):
        rows = pl.ds(pl.multiple_of(i * BLOCK, BLOCK), BLOCK)
        output = dot(hidden[...], w_out[...])
        fresh = normalize(output, gain[level, 0:1, :], bias[level, 0:1, :])
        fresh = (edges[rows, :].astype(F32) + fresh).astype(BF16)
        if keep:
            fresh_edges[rows, :] = fresh
        total[...] += dot(hot_columns(receivers[:, rows], node_count).astype(BF16), fresh)

    def both(i, ready, filling):
        pre_copy(i + 1).wait()
        edge_copy(i).wait()
        gather(i + 1, filling)
        update(i, ready)
        if keep:
            fresh_copy(i).start()

    pre_copy(0).wait()
    gather(0, hidden_0)
    for copy in second:
        copy.wait()

    def step(pair, _):
        both(2 * pair, hidden_0, hidden_1)
        both(2 * pair + 1, hidden_1, hidden_0)
        return 0

    lax.fori_loop(0, blocks // 2 - 1, step, 0)
    both(blocks - 2, hidden_0, hidden_1)
    edge_copy(blocks - 1).wait()
    update(blocks - 1, hidden_1)
    if keep:
        fresh_copy(blocks - 1).start()

    for copy in third:
        copy.wait()
    here = nodes[...]
    pre_node = dot(here, w_node[0]) + dot(total[...].astype(BF16), w_node[1])
    output = dot(silu(pre_node).astype(BF16), w_node_out[...])
    updated = here.astype(F32) + normalize(output, gain[level, 1:2, :], bias[level, 1:2, :])
    updated = updated.astype(BF16)
    new_nodes[...] = updated
    ends = [begin(new_nodes, new_nodes_h, sems.at[12])]
    if not last:
        sent = project(updated, w_next[...])
        outgoing[...] = sent
        ends.append(begin(outgoing, outgoing_h, sems.at[13]))
        for i in range(out_rows.shape[0] // BLOCK):
            rows = pl.ds(i * BLOCK, BLOCK)
            out_rows[rows, :] = dot(picks[rows, :], sent).astype(BF16)
            ends.append(begin(out_rows.at[rows], out_rows_h.at[rows], pre_sems.at[i]))
    if keep:
        for i in range(blocks):
            fresh_copy(i).wait()
    for copy in ends:
        copy.wait()


HBM = pl.BlockSpec(memory_space=pltpu.HBM)
VMEM = pl.BlockSpec(memory_space=pltpu.VMEM)


def pre_stage(level, edges, receivers, nodes, edge_in, extra=(), shape=None):
    edge_count, width = edges.shape
    node_count = nodes.shape[0]
    blocks = edge_count // BLOCK
    operands = [edges, receivers, nodes, edge_in, *extra]
    out_shape = [pltpu.HBM((edge_count, width), F32)]
    line = pltpu.VMEM((1, edge_count), I32)
    weight = pltpu.VMEM((width, width), BF16)
    scratch = [
        pltpu.VMEM((edge_count, width), BF16), line, pltpu.VMEM((node_count, width), BF16),
        weight, weight, pltpu.VMEM((edge_count, width), F32),
    ]
    if shape:
        tile, send_rows = extra[:2]
        out_shape += [
            pltpu.HBM(tile.shape, BF16),
            pltpu.HBM((send_rows.shape[1], node_count), BF16),
            pltpu.HBM((1, edge_count), I32),
            pltpu.HBM((1, edge_count), I32),
        ]
        tiled = pltpu.VMEM(tile.shape, BF16)
        scratch += [
            tiled, weight, pltpu.VMEM(send_rows.shape, I32), line, line, tiled,
            pltpu.VMEM((send_rows.shape[1], node_count), BF16), line, line,
        ]
    scratch += [pltpu.SemaphoreType.DMA((n,)) for n in (13, blocks, blocks)]
    return pl.pallas_call(
        functools.partial(pre_kernel, level, shape),
        out_shape=out_shape,
        in_specs=[HBM] * len(operands),
        out_specs=[HBM] * len(out_shape),
        scratch_shapes=scratch,
        name="pre_first" if shape else "pre_next",
        cost_estimate=pl.CostEstimate(
            flops=2 * edge_count * width * (width + node_count),
            bytes_accessed=edge_count * width * 6,
            transcendentals=0,
        ),
        compiler_params=pltpu.CompilerParams(vmem_limit_bytes=20 * MIB),
    )(*[pltpu.with_memory_space_constraint(operand, pltpu.HBM) for operand in operands])


def main_stage(level, places, receivers, pre, edges, nodes, weights, tables, picks, last, keep):
    edge_count, width = edges.shape
    node_count = nodes.shape[0]
    operands = [places, receivers, pre, edges, nodes, *weights, *tables]
    in_specs = [HBM] * 12 + [VMEM] * (len(tables) - 1)
    out_shape = [pltpu.HBM((node_count, width), BF16)]
    blocks = edge_count // BLOCK
    table_rows = sum(piece.shape[0] for piece in tables)
    norm = pltpu.VMEM(weights[4].shape, F32)
    small = pltpu.VMEM((node_count, width), BF16)
    weight = pltpu.VMEM((width, width), BF16)
    scratch = [
        pltpu.VMEM((table_rows * (width // LANES), LANES), F32),
        pltpu.VMEM((BLOCK, width), BF16),
        pltpu.VMEM((BLOCK, width), BF16),
        pltpu.VMEM((node_count, width), F32),
        pltpu.SMEM((1, edge_count), I32),
        pltpu.VMEM((1, edge_count), I32),
        pltpu.VMEM((edge_count, width), F32),
        pltpu.VMEM((edge_count, width), BF16),
        small, weight, pltpu.VMEM((2, width, width), BF16), weight, norm, norm, small,
        pltpu.VMEM(tables[0].shape, BF16),
    ]
    if len(tables) > 2:
        scratch.append(weight)
    if not last:
        operands.append(picks)
        in_specs.append(HBM)
        rows = picks.shape[0]
        out_shape.append(pltpu.HBM((node_count, width), BF16))
        out_shape.append(pltpu.HBM((rows, width), BF16))
        scratch += [weight, pltpu.VMEM(picks.shape, BF16), small, pltpu.VMEM((rows, width), BF16)]
    if keep:
        out_shape.append(pltpu.HBM((edge_count, width), BF16))
        scratch.append(pltpu.VMEM((edge_count, width), BF16))
    scratch += [pltpu.SemaphoreType.DMA((n,)) for n in (14, blocks, blocks, blocks)]
    operands = [
        pltpu.with_memory_space_constraint(operand, pltpu.HBM) if spec is HBM else operand
        for operand, spec in zip(operands, in_specs)
    ]
    return pl.pallas_call(
        functools.partial(main_kernel, level, len(tables), last, keep),
        out_shape=out_shape,
        in_specs=in_specs,
        out_specs=[HBM] * len(out_shape),
        scratch_shapes=scratch,
        name="encode" if level == 0 else "layer",
        cost_estimate=pl.CostEstimate(
            flops=2 * edge_count * width * (width + node_count),
            bytes_accessed=edge_count * width * 10,
            transcendentals=edge_count * width,
        ),
        compiler_params=pltpu.CompilerParams(vmem_limit_bytes=32 * MIB),
    )(*operands)


def shift(array, axis, step, wrap):
    size = lax.axis_size(axis)
    pairs = [(i, (i + step) % size) for i in range(size) if wrap or 0 <= i + step < size]
    return lax.ppermute(array, axis, pairs)


def local(
    grid_latent,
    mesh_latent,
    g2m_edges,
    g2m_senders,
    g2m_receivers,
    mm_edges,
    mm_senders,
    mm_receivers,
    send_rows,
    edge_in,
    edge_out,
    node_in,
    node_out,
    norm_gain,
    norm_bias,
):
    high, wide, features = grid_latent.shape
    flat_tile = grid_latent.reshape(high * wide, features)
    weights = [edge_in, edge_out, node_in, node_out, norm_gain, norm_bias]

    north = shift(grid_latent, "lat", 1, False)
    south = shift(grid_latent, "lat", -1, False)
    pre, tile_terms, picks, places, lines = pre_stage(
        0, g2m_edges, g2m_receivers, mesh_latent, edge_in,
        (flat_tile, send_rows, g2m_senders, mm_senders), (high, wide),
    )
    north, south, tile_terms = lax.optimization_barrier((north, south, tile_terms))

    def column(first):
        pieces = [piece[:, first:first + HALO] for piece in (north, grid_latent, south)]
        return jnp.concatenate(pieces, axis=0).reshape(-1, features)

    west = shift(column(wide - HALO), "lon", 1, True)
    east = shift(column(0), "lon", -1, True)
    tables = [tile_terms, north.reshape(-1, features), south.reshape(-1, features), west, east]
    nodes, outgoing, out_rows = main_stage(
        0, places, g2m_receivers, pre, g2m_edges, mesh_latent, weights, tables, picks, False, False
    )
    edges = mm_edges
    levels = edge_in.shape[0]
    devices = lax.axis_size("lat") * lax.axis_size("lon")
    for level in range(1, levels):
        blocks = out_rows.reshape(devices, -1, features)
        arrived = lax.all_to_all(blocks, ("lat", "lon"), split_axis=0, concat_axis=0, tiled=True)
        arrived = arrived.reshape(-1, features)
        (pre,) = pre_stage(level, edges, mm_receivers, nodes, edge_in)
        last = level == levels - 1
        results = main_stage(
            level, lines, mm_receivers, pre, edges, nodes, weights, [outgoing, arrived], picks,
            last, not last,
        )
        if last:
            (nodes,) = results
        else:
            nodes, outgoing, out_rows, edges = results
    return nodes


def solution(mesh):
    in_specs = (
        P("lat", "lon", None),
        P(("lat", "lon"), None),
        P(("lat", "lon"), None),
        P(("lat", "lon"), None),
        P(("lat", "lon"), None),
        P(("lat", "lon"), None),
        P(("lat", "lon"), None),
        P(("lat", "lon"), None),
        P(("lat", "lon"), None),
        P(),
        P(),
        P(),
        P(),
        P(),
        P(),
    )
    out_specs = P(("lat", "lon"), None)
    return jax.shard_map(local, mesh=mesh, in_specs=in_specs, out_specs=out_specs, check_vma=False)
```

```python
import functools

import jax
import jax.numpy as jnp
from jax import lax
from jax.experimental import pallas as pl
from jax.experimental.pallas import tpu as pltpu
from jax.sharding import PartitionSpec as P

HALO = 4
NORM_EPS = 1e-05
F32 = jnp.float32
BF16 = jnp.bfloat16
I32 = jnp.int32
BLOCK = 256
CHUNK = 256
GROUP = 16
PRE_BLOCK = 512
LANES = 128
MIB = 1024 * 1024


def silu_of_half(half):
    return half + half * jnp.tanh(half)


def normalize(values, gains, biases):
    centre = jnp.mean(values, axis=-1, keepdims=True)
    shifted = values - centre
    spread = jnp.mean(shifted * shifted, axis=-1, keepdims=True)
    return shifted * lax.rsqrt(spread + NORM_EPS) * gains + biases


def dot(left, right):
    return jnp.dot(left, right, preferred_element_type=F32)


def project(values, weights):
    return dot(values, weights).astype(BF16)


def hot_columns(indices, nodes):
    places = lax.broadcasted_iota(I32, (nodes, indices.shape[1]), 0)
    return jnp.where(places == indices, 1.0, 0.0)


def hot_rows(indices, nodes):
    return hot_columns(indices, nodes).T.astype(BF16)


def cell_row(cell, high, wide):
    across = wide + 2 * HALO
    row = (cell * 241) >> 15
    column = cell - row * across
    band = jnp.where(row < HALO, 1, jnp.where(row < HALO + high, 0, 2))
    inner = row - jnp.where(band == 1, 0, jnp.where(band == 0, HALO, HALO + high))
    cells = high * wide
    tall = (high + 2 * HALO) * HALO
    side = 3 * cells + row * HALO
    west = side + column
    east = side + tall + column - HALO - wide
    centre = band * cells + inner * wide + column - HALO
    return jnp.where(column < HALO, west, jnp.where(column < HALO + wide, centre, east))


def begin(source, target, sem):
    copy = pltpu.make_async_copy(source, target, sem)
    copy.start()
    return copy


def part(ref, i, size=BLOCK):
    return ref.at[pl.ds(pl.multiple_of(i * size, size), size)]


def pre_kernel(level, shape, edges_h, receivers_h, nodes_h, edge_in_h, *refs):
    refs = list(refs)
    take = lambda count: [refs.pop(0) for _ in range(count)]
    if shape:
        tile_h, cells_h, senders_h = take(3)
    pre_h = take(1)[0]
    if shape:
        tile_terms_h, places_h, lines_h = take(3)
    edges, receivers, nodes, w_edge, w_recv, pre = take(6)
    if shape:
        tile, w_send, cells, senders, tile_terms, places, lines = take(7)
    sems, edge_sems, out_sems = take(3)
    node_count = nodes.shape[0]
    blocks = edges.shape[0] // PRE_BLOCK

    def edge_copy(i):
        return pltpu.make_async_copy(part(edges_h, i, PRE_BLOCK), part(edges, i, PRE_BLOCK), edge_sems.at[i])

    def out_copy(i):
        return pltpu.make_async_copy(part(pre, i, PRE_BLOCK), part(pre_h, i, PRE_BLOCK), out_sems.at[i])

    first = [
        begin(nodes_h, nodes, sems.at[0]),
        begin(edge_in_h.at[level, 2], w_recv, sems.at[1]),
        begin(receivers_h, receivers, sems.at[2]),
        begin(edge_in_h.at[level, 0], w_edge, sems.at[3]),
    ]
    edge_copy(0).start()
    if shape:
        second = [
            begin(tile_h, tile, sems.at[4]),
            begin(edge_in_h.at[level, 1], w_send, sems.at[5]),
            begin(cells_h, cells, sems.at[6]),
            begin(senders_h, senders, sems.at[7]),
        ]
    for i in range(1, blocks):
        edge_copy(i).start()
    for copy in first:
        copy.wait()
    terms = project(nodes[...], w_recv[...])

    def step(i, _):
        rows = pl.ds(pl.multiple_of(i * PRE_BLOCK, PRE_BLOCK), PRE_BLOCK)
        edge_copy(i).wait()
        hot = hot_rows(jnp.minimum(receivers[:, rows], node_count - 1), node_count)
        pre[rows, :] = 0.5 * (dot(edges[rows, :], w_edge[...]) + dot(hot, terms))
        out_copy(i).start()
        return 0

    lax.fori_loop(0, blocks, step, 0)
    if shape:
        high, wide = shape
        tiles = edges.shape[1] // LANES
        for copy in second:
            copy.wait()
        tile_terms[...] = project(tile[...], w_send[...])
        ends = [begin(tile_terms, tile_terms_h, sems.at[8])]
        places[...] = cell_row(cells[...], high, wide) * tiles
        lines[...] = senders[...] * tiles
        ends.append(begin(places, places_h, sems.at[9]))
        ends.append(begin(lines, lines_h, sems.at[10]))
    for i in range(blocks):
        out_copy(i).wait()
    if shape:
        for copy in ends:
            copy.wait()


def halo_kernel(node_count, north, south, send_rows_h, edge_in_h, terms, picks_h, send_rows, w_send, picks, sems):
    copies = [
        begin(edge_in_h.at[0, 1], w_send, sems.at[0]),
        begin(send_rows_h, send_rows, sems.at[1]),
    ]
    for copy in copies:
        copy.wait()
    size = north.shape[0]
    terms[0:size, :] = project(north[...], w_send[...])
    terms[size:2 * size, :] = project(south[...], w_send[...])

    def pick(i, _):
        rows = pl.ds(pl.multiple_of(i * BLOCK, BLOCK), BLOCK)
        picks[rows, :] = hot_rows(send_rows[:, rows], node_count)
        return 0

    lax.fori_loop(0, picks.shape[0] // BLOCK, pick, 0)
    begin(picks, picks_h, sems.at[2]).wait()


def fill_table(table, start, values):
    tiles = values.shape[1] // LANES
    for group in range(values.shape[0] // 8):
        for tile in range(tiles):
            lines = pl.ds((start + group * 8) * tiles + tile, 8, stride=tiles)
            table[lines, :] = values[group * 8:group * 8 + 8, tile * LANES:(tile + 1) * LANES]


def main_kernel(level, raw, last, keep, *refs):
    refs = list(refs)
    take = lambda count: [refs.pop(0) for _ in range(count)]
    places_h, receivers_h, pre_h, edges_h, nodes_h = take(5)
    edge_in_h, edge_out_h, node_in_h, node_out_h, gain_h, bias_h = take(6)
    local_h, rows_in = take(2)
    raw_rows = take(raw)
    picks_h = None if last else take(1)[0]
    new_nodes_h = take(1)[0]
    outgoing_h, out_rows_h = (None, None) if last else take(2)
    new_edges_h = take(1)[0] if keep else None
    table, stage_0, stage_1, hidden_0, hidden_1, output_0, output_1 = take(7)
    total, places, receivers, pre, edges = take(5)
    nodes, w_out, w_node, w_node_out, gain, bias, new_nodes, local_rows, fresh_edges = take(9)
    w_send = take(1)[0] if raw else None
    w_next, picks, outgoing, out_rows = (None,) * 4 if last else take(4)
    sems, pre_sems, edge_sems, out_sems = take(4)

    node_count, width = nodes.shape
    blocks = edges.shape[0] // BLOCK
    tiles = width // LANES
    stages = [stage_0, stage_1]
    hidden = [hidden_0, hidden_1]
    outputs = [output_0, output_1]

    def pre_copy(i):
        return pltpu.make_async_copy(part(pre_h, i), part(pre, i), pre_sems.at[i])

    def edge_copy(i):
        return pltpu.make_async_copy(part(edges_h, i), part(edges, i), edge_sems.at[i])

    def fresh_copy(i):
        return pltpu.make_async_copy(part(fresh_edges, i), part(new_edges_h, i), out_sems.at[i])

    places_copy = begin(places_h, places, sems.at[1])
    local_copy = begin(local_h, local_rows, sems.at[0])
    if raw:
        send_copy = begin(edge_in_h.at[level, 1], w_send, sems.at[2])
    pre_copy(0).start()
    second = [
        begin(edge_out_h.at[level], w_out, sems.at[3]),
        begin(receivers_h, receivers, sems.at[4]),
        begin(gain_h, gain, sems.at[5]),
        begin(bias_h, bias, sems.at[6]),
    ]
    pre_copy(1).start()
    for i in range(blocks):
        edge_copy(i).start()
        if i + 2 < blocks:
            pre_copy(i + 2).start()
    third = [
        begin(nodes_h, nodes, sems.at[7]),
        begin(node_in_h.at[level], w_node, sems.at[8]),
        begin(node_out_h.at[level], w_node_out, sems.at[9]),
    ]
    if not last:
        third.append(begin(edge_in_h.at[level + 1, 1], w_next, sems.at[10]))
        third.append(begin(picks_h, picks, sems.at[11]))

    total[...] = jnp.zeros_like(total)
    start = local_rows.shape[0]
    for at in range(0, rows_in.shape[0], CHUNK):
        fill_table(table, start + at, rows_in[at:at + CHUNK, :].astype(F32) * 0.5)
    start += rows_in.shape[0]
    local_copy.wait()
    fill_table(table, 0, local_rows[...].astype(F32) * 0.5)
    if raw:
        send_copy.wait()
    for source in raw_rows:
        fill_table(table, start, project(source[...], w_send[...]).astype(F32) * 0.5)
        start += source.shape[0]
    places_copy.wait()

    def found(at):
        stage = stages[at // BLOCK % 2]
        base = at % BLOCK * tiles
        for j in range(8):
            stage[base + j * tiles:base + (j + 1) * tiles, :] = table[pl.ds(places[0, at + j], tiles), :]
        return [stage[pl.ds(base + tile, 8, stride=tiles), :] for tile in range(tiles)]

    def gather(i, group):
        halves = []
        for at in range(i * BLOCK + group * GROUP, i * BLOCK + (group + 1) * GROUP, 8):
            rows = found(at)
            halves.append([
                silu_of_half(pre[at:at + 8, t * LANES:(t + 1) * LANES] + rows[t]) for t in range(tiles)
            ])
        for t in range(tiles):
            both = jnp.concatenate([half[t] for half in halves], axis=0).astype(BF16)
            hidden[i % 2][group * GROUP:(group + 1) * GROUP, t * LANES:(t + 1) * LANES] = both

    def settle(i, group):
        rows = slice(i * BLOCK + group * GROUP, i * BLOCK + (group + 1) * GROUP)
        output = outputs[i % 2][group * GROUP:(group + 1) * GROUP, :]
        fresh = normalize(output, gain[level, 0:1, :], bias[level, 0:1, :])
        fresh_edges[rows, :] = (edges[rows, :].astype(F32) + fresh).astype(BF16)

    for turn in range(-2, blocks + 1):
        gathering = turn + 2 if turn + 2 < blocks else None
        multiplying = turn + 1 if 0 <= turn + 1 < blocks else None
        settling = turn if 0 <= turn < blocks else None
        adding = turn - 1 if turn >= 1 else None
        if gathering is not None:
            pre_copy(gathering).wait()
        if settling is not None:
            edge_copy(settling).wait()
        if turn == -1:
            for copy in second:
                copy.wait()
        if keep and adding is not None:
            fresh_copy(adding).start()
        if multiplying is not None:
            outputs[multiplying % 2][...] = dot(hidden[multiplying % 2][...], w_out[...])
        if adding is not None:
            rows = slice(adding * BLOCK, (adding + 1) * BLOCK)
            hot = hot_columns(receivers[:, rows], node_count).astype(BF16)
            total[...] += dot(hot, fresh_edges[rows, :])
        for group in range(BLOCK // GROUP):
            if gathering is not None:
                gather(gathering, group)
            if settling is not None:
                settle(settling, group)

    for copy in third:
        copy.wait()
    here = nodes[...]
    pre_node = dot(here, w_node[0]) + dot(total[...].astype(BF16), w_node[1])
    output = dot(silu_of_half(pre_node * 0.5).astype(BF16), w_node_out[...])
    updated = here.astype(F32) + normalize(output, gain[level, 1:2, :], bias[level, 1:2, :])
    updated = updated.astype(BF16)
    new_nodes[...] = updated
    ends = [begin(new_nodes, new_nodes_h, sems.at[12])]
    if not last:
        sent = project(updated, w_next[...])
        outgoing[...] = sent
        ends.append(begin(outgoing, outgoing_h, sems.at[13]))
        for i in range(out_rows.shape[0] // BLOCK):
            rows = pl.ds(i * BLOCK, BLOCK)
            out_rows[rows, :] = dot(picks[rows, :], sent).astype(BF16)
            ends.append(begin(out_rows.at[rows], out_rows_h.at[rows], pre_sems.at[i]))
    if keep:
        for i in range(blocks):
            fresh_copy(i).wait()
    for copy in ends:
        copy.wait()


HBM = pl.BlockSpec(memory_space=pltpu.HBM)
VMEM = pl.BlockSpec(memory_space=pltpu.VMEM)


def pinned(operands, specs):
    pin = pltpu.with_memory_space_constraint
    return [pin(operand, pltpu.HBM) if spec is HBM else operand for operand, spec in zip(operands, specs)]


def pre_stage(level, edges, receivers, nodes, edge_in, extra=(), shape=None):
    edge_count, width = edges.shape
    node_count = nodes.shape[0]
    blocks = edge_count // PRE_BLOCK
    operands = [edges, receivers, nodes, edge_in, *extra]
    out_shape = [pltpu.HBM((edge_count, width), F32)]
    line = pltpu.VMEM((1, edge_count), I32)
    weight = pltpu.VMEM((width, width), BF16)
    scratch = [
        pltpu.VMEM((edge_count, width), BF16), line, pltpu.VMEM((node_count, width), BF16),
        weight, weight, pltpu.VMEM((edge_count, width), F32),
    ]
    if shape:
        tile = extra[0]
        out_shape += [
            pltpu.HBM(tile.shape, BF16), pltpu.HBM((1, edge_count), I32), pltpu.HBM((1, edge_count), I32),
        ]
        tiled = pltpu.VMEM(tile.shape, BF16)
        scratch += [tiled, weight, line, line, tiled, line, line]
    scratch += [pltpu.SemaphoreType.DMA((n,)) for n in (11, blocks, blocks)]
    in_specs = [HBM] * len(operands)
    return pl.pallas_call(
        functools.partial(pre_kernel, level, shape),
        out_shape=out_shape,
        in_specs=in_specs,
        out_specs=[HBM] * len(out_shape),
        scratch_shapes=scratch,
        name="pre_first" if shape else "pre_next",
        cost_estimate=pl.CostEstimate(
            flops=2 * edge_count * width * (width + node_count),
            bytes_accessed=edge_count * width * 6,
            transcendentals=0,
        ),
        compiler_params=pltpu.CompilerParams(vmem_limit_bytes=20 * MIB),
    )(*pinned(operands, in_specs))


def halo_stage(north, south, send_rows, edge_in, node_count):
    rows, width = north.shape
    count = send_rows.shape[1]
    in_specs = [VMEM, VMEM, HBM, HBM]
    return pl.pallas_call(
        functools.partial(halo_kernel, node_count),
        out_shape=[jax.ShapeDtypeStruct((2 * rows, width), BF16), pltpu.HBM((count, node_count), BF16)],
        in_specs=in_specs,
        out_specs=[VMEM, HBM],
        scratch_shapes=[
            pltpu.VMEM((1, count), I32), pltpu.VMEM((width, width), BF16),
            pltpu.VMEM((count, node_count), BF16), pltpu.SemaphoreType.DMA((3,)),
        ],
        name="halo_terms",
        cost_estimate=pl.CostEstimate(
            flops=4 * rows * width * width, bytes_accessed=6 * rows * width, transcendentals=0
        ),
        compiler_params=pltpu.CompilerParams(vmem_limit_bytes=8 * MIB),
    )(*pinned([north, south, send_rows, edge_in], in_specs))


def main_stage(level, places, receivers, pre, edges, nodes, weights, tables, picks, last, keep):
    edge_count, width = edges.shape
    node_count = nodes.shape[0]
    operands = [places, receivers, pre, edges, nodes, *weights, *tables]
    in_specs = [HBM] * 12 + [VMEM] * (len(tables) - 1)
    out_shape = [pltpu.HBM((node_count, width), BF16)]
    blocks = edge_count // BLOCK
    table_rows = sum(piece.shape[0] for piece in tables)
    norm = pltpu.VMEM(weights[4].shape, F32)
    small = pltpu.VMEM((node_count, width), BF16)
    weight = pltpu.VMEM((width, width), BF16)
    scratch = [
        pltpu.VMEM((table_rows * (width // LANES), LANES), F32),
        pltpu.VMEM((BLOCK * (width // LANES), LANES), F32),
        pltpu.VMEM((BLOCK * (width // LANES), LANES), F32),
        pltpu.VMEM((BLOCK, width), BF16),
        pltpu.VMEM((BLOCK, width), BF16),
        pltpu.VMEM((BLOCK, width), F32),
        pltpu.VMEM((BLOCK, width), F32),
        pltpu.VMEM((node_count, width), F32),
        pltpu.SMEM((1, edge_count), I32),
        pltpu.VMEM((1, edge_count), I32),
        pltpu.VMEM((edge_count, width), F32),
        pltpu.VMEM((edge_count, width), BF16),
        small, weight, pltpu.VMEM((2, width, width), BF16), weight, norm, norm, small,
        pltpu.VMEM(tables[0].shape, BF16), pltpu.VMEM((edge_count, width), BF16),
    ]
    raw = len(tables) - 2
    if raw:
        scratch.append(weight)
    if not last:
        operands.append(picks)
        in_specs.append(HBM)
        rows = picks.shape[0]
        out_shape += [pltpu.HBM((node_count, width), BF16), pltpu.HBM((rows, width), BF16)]
        scratch += [weight, pltpu.VMEM(picks.shape, BF16), small, pltpu.VMEM((rows, width), BF16)]
    if keep:
        out_shape.append(pltpu.HBM((edge_count, width), BF16))
    scratch += [pltpu.SemaphoreType.DMA((n,)) for n in (14, blocks, blocks, blocks)]
    return pl.pallas_call(
        functools.partial(main_kernel, level, raw, last, keep),
        out_shape=out_shape,
        in_specs=in_specs,
        out_specs=[HBM] * len(out_shape),
        scratch_shapes=scratch,
        name="encode" if level == 0 else "layer",
        cost_estimate=pl.CostEstimate(
            flops=2 * edge_count * width * (width + node_count),
            bytes_accessed=edge_count * width * 10,
            transcendentals=edge_count * width,
        ),
        compiler_params=pltpu.CompilerParams(vmem_limit_bytes=32 * MIB),
    )(*pinned(operands, in_specs))


def shift(array, axis, step, wrap):
    size = lax.axis_size(axis)
    pairs = [(i, (i + step) % size) for i in range(size) if wrap or 0 <= i + step < size]
    return lax.ppermute(array, axis, pairs)


def local(
    grid_latent,
    mesh_latent,
    g2m_edges,
    g2m_senders,
    g2m_receivers,
    mm_edges,
    mm_senders,
    mm_receivers,
    send_rows,
    edge_in,
    edge_out,
    node_in,
    node_out,
    norm_gain,
    norm_bias,
):
    high, wide, features = grid_latent.shape
    flat_tile = grid_latent.reshape(high * wide, features)
    weights = [edge_in, edge_out, node_in, node_out, norm_gain, norm_bias]

    north = shift(grid_latent, "lat", 1, False)
    south = shift(grid_latent, "lat", -1, False)
    pre, tile_terms, places, lines = pre_stage(
        0, g2m_edges, g2m_receivers, mesh_latent, edge_in,
        (flat_tile, g2m_senders, mm_senders), (high, wide),
    )
    north, south, tile_terms = lax.optimization_barrier((north, south, tile_terms))

    def column(first):
        pieces = [piece[:, first:first + HALO] for piece in (north, grid_latent, south)]
        return jnp.concatenate(pieces, axis=0).reshape(-1, features)

    west = shift(column(wide - HALO), "lon", 1, True)
    east = shift(column(0), "lon", -1, True)
    halo_terms, picks = halo_stage(
        north.reshape(-1, features), south.reshape(-1, features), send_rows, edge_in, mesh_latent.shape[0]
    )
    tables = [tile_terms, halo_terms, west, east]
    nodes, outgoing, out_rows = main_stage(
        0, places, g2m_receivers, pre, g2m_edges, mesh_latent, weights, tables, picks, False, False
    )
    edges = mm_edges
    levels = edge_in.shape[0]
    devices = lax.axis_size("lat") * lax.axis_size("lon")
    for level in range(1, levels):
        blocks = out_rows.reshape(devices, -1, features)
        arrived = lax.all_to_all(blocks, ("lat", "lon"), split_axis=0, concat_axis=0, tiled=True)
        arrived = arrived.reshape(-1, features)
        (pre,) = pre_stage(level, edges, mm_receivers, nodes, edge_in)
        last = level == levels - 1
        results = main_stage(
            level, lines, mm_receivers, pre, edges, nodes, weights, [outgoing, arrived], picks,
            last, not last,
        )
        if last:
            (nodes,) = results
        else:
            nodes, outgoing, out_rows, edges = results
    return nodes


def solution(mesh):
    in_specs = (
        P("lat", "lon", None),
        P(("lat", "lon"), None),
        P(("lat", "lon"), None),
        P(("lat", "lon"), None),
        P(("lat", "lon"), None),
        P(("lat", "lon"), None),
        P(("lat", "lon"), None),
        P(("lat", "lon"), None),
        P(("lat", "lon"), None),
        P(),
        P(),
        P(),
        P(),
        P(),
        P(),
    )
    out_specs = P(("lat", "lon"), None)
    return jax.shard_map(local, mesh=mesh, in_specs=in_specs, out_specs=out_specs, check_vma=False)
```

```python
import functools

import jax
import jax.numpy as jnp
from jax import lax
from jax.experimental import pallas as pl
from jax.experimental.pallas import tpu as pltpu
from jax.sharding import PartitionSpec as P

HALO = 4
NORM_EPS = 1e-05
F32 = jnp.float32
BF16 = jnp.bfloat16
I32 = jnp.int32
BLOCK = 512
CHUNK = 256
GROUP = 32
PRE_BLOCK = 512
PICK_BLOCK = 256
LANES = 128
MIB = 1024 * 1024


def silu_of_half(half):
    return half + half * jnp.tanh(half)


def normalize(values, gains, biases):
    centre = jnp.mean(values, axis=-1, keepdims=True)
    shifted = values - centre
    spread = jnp.mean(shifted * shifted, axis=-1, keepdims=True)
    return shifted * lax.rsqrt(spread + NORM_EPS) * gains + biases


def dot(left, right):
    return jnp.dot(left, right, preferred_element_type=F32)


def project(values, weights):
    return dot(values, weights).astype(BF16)


def hot_columns(indices, nodes):
    places = lax.broadcasted_iota(I32, (nodes, indices.shape[1]), 0)
    return jnp.where(places == indices, 1.0, 0.0)


def hot_rows(indices, nodes):
    return hot_columns(indices, nodes).T.astype(BF16)


def cell_row(cell, high, wide):
    across = wide + 2 * HALO
    row = (cell * 241) >> 15
    column = cell - row * across
    band = jnp.where(row < HALO, 1, jnp.where(row < HALO + high, 0, 2))
    inner = row - jnp.where(band == 1, 0, jnp.where(band == 0, HALO, HALO + high))
    cells = high * wide
    tall = (high + 2 * HALO) * HALO
    side = 3 * cells + row * HALO
    west = side + column
    east = side + tall + column - HALO - wide
    centre = band * cells + inner * wide + column - HALO
    return jnp.where(column < HALO, west, jnp.where(column < HALO + wide, centre, east))


def begin(source, target, sem):
    copy = pltpu.make_async_copy(source, target, sem)
    copy.start()
    return copy


def part(ref, i, size=BLOCK):
    return ref.at[pl.ds(pl.multiple_of(i * size, size), size)]


def pre_kernel(level, shape, edges_h, receivers_h, nodes_h, edge_in_h, *refs):
    refs = list(refs)
    take = lambda count: [refs.pop(0) for _ in range(count)]
    if shape:
        tile_h, cells_h, senders_h, send_rows_h = take(4)
    pre_h = take(1)[0]
    if shape:
        tile_terms_h, places_h, lines_h, picks_h = take(4)
    edges, receivers, nodes, w_edge, w_recv, pre = take(6)
    if shape:
        tile, w_send, cells, senders, tile_terms, places, lines, send_rows, picks = take(9)
    sems, edge_sems, out_sems = take(3)
    node_count = nodes.shape[0]
    blocks = edges.shape[0] // PRE_BLOCK

    def edge_copy(i):
        return pltpu.make_async_copy(part(edges_h, i, PRE_BLOCK), part(edges, i, PRE_BLOCK), edge_sems.at[i])

    def out_copy(i):
        return pltpu.make_async_copy(part(pre, i, PRE_BLOCK), part(pre_h, i, PRE_BLOCK), out_sems.at[i])

    first = [
        begin(nodes_h, nodes, sems.at[0]),
        begin(edge_in_h.at[level, 2], w_recv, sems.at[1]),
        begin(receivers_h, receivers, sems.at[2]),
        begin(edge_in_h.at[level, 0], w_edge, sems.at[3]),
    ]
    edge_copy(0).start()
    if shape:
        second = [
            begin(tile_h, tile, sems.at[4]),
            begin(edge_in_h.at[level, 1], w_send, sems.at[5]),
            begin(cells_h, cells, sems.at[6]),
            begin(senders_h, senders, sems.at[7]),
            begin(send_rows_h, send_rows, sems.at[11]),
        ]
    for i in range(1, blocks):
        edge_copy(i).start()
    for copy in first:
        copy.wait()
    terms = project(nodes[...], w_recv[...])

    def step(i, _):
        rows = pl.ds(pl.multiple_of(i * PRE_BLOCK, PRE_BLOCK), PRE_BLOCK)
        edge_copy(i).wait()
        hot = hot_rows(jnp.minimum(receivers[:, rows], node_count - 1), node_count)
        pre[rows, :] = 0.5 * (dot(edges[rows, :], w_edge[...]) + dot(hot, terms))
        out_copy(i).start()
        return 0

    lax.fori_loop(0, blocks, step, 0)
    if shape:
        high, wide = shape
        tiles = edges.shape[1] // LANES
        for copy in second:
            copy.wait()

        def pick(i, _):
            rows = pl.ds(pl.multiple_of(i * PRE_BLOCK, PRE_BLOCK), PRE_BLOCK)
            picks[rows, :] = hot_rows(send_rows[:, rows], node_count)
            return 0

        lax.fori_loop(0, picks.shape[0] // PRE_BLOCK, pick, 0)
        tile_terms[...] = project(tile[...], w_send[...])
        ends = [begin(tile_terms, tile_terms_h, sems.at[8])]
        places[...] = cell_row(cells[...], high, wide) * tiles
        lines[...] = senders[...] * tiles
        ends.append(begin(places, places_h, sems.at[9]))
        ends.append(begin(lines, lines_h, sems.at[10]))
        ends.append(begin(picks, picks_h, sems.at[12]))
    for i in range(blocks):
        out_copy(i).wait()
    if shape:
        for copy in ends:
            copy.wait()


def halo_kernel(north, south, edge_in_h, terms, w_send, sem):
    begin(edge_in_h.at[0, 1], w_send, sem).wait()
    size = north.shape[0]
    terms[0:size, :] = project(north[...], w_send[...])
    terms[size:2 * size, :] = project(south[...], w_send[...])


def fill_table(table, start, values):
    tiles = values.shape[1] // LANES
    for group in range(values.shape[0] // 8):
        for tile in range(tiles):
            lines = pl.ds((start + group * 8) * tiles + tile, 8, stride=tiles)
            table[lines, :] = values[group * 8:group * 8 + 8, tile * LANES:(tile + 1) * LANES]


def main_kernel(level, raw, last, keep, *refs):
    refs = list(refs)
    take = lambda count: [refs.pop(0) for _ in range(count)]
    places_h, receivers_h, pre_h, edges_h, nodes_h = take(5)
    edge_in_h, edge_out_h, node_in_h, node_out_h, gain_h, bias_h = take(6)
    local_h, rows_in = take(2)
    raw_rows = take(raw)
    picks_h = None if last else take(1)[0]
    new_nodes_h = take(1)[0]
    outgoing_h, out_rows_h = (None, None) if last else take(2)
    new_edges_h = take(1)[0] if keep else None
    table, stage_0, stage_1, hidden_0, hidden_1, output_0, output_1 = take(7)
    total, places, receivers, pre, edges = take(5)
    nodes, w_out, w_node, w_node_out, gain, bias, new_nodes, local_rows, fresh_edges = take(9)
    w_send = take(1)[0] if raw else None
    w_next, picks, outgoing, out_rows = (None,) * 4 if last else take(4)
    sems, pre_sems, edge_sems, out_sems, pick_sems = take(5)

    node_count, width = nodes.shape
    blocks = edges.shape[0] // BLOCK
    tiles = width // LANES
    stages = [stage_0, stage_1]
    hidden = [hidden_0, hidden_1]
    outputs = [output_0, output_1]

    def pre_copy(i):
        return pltpu.make_async_copy(part(pre_h, i), part(pre, i), pre_sems.at[i])

    def edge_copy(i):
        return pltpu.make_async_copy(part(edges_h, i), part(edges, i), edge_sems.at[i])

    def fresh_copy(i):
        return pltpu.make_async_copy(part(fresh_edges, i), part(new_edges_h, i), out_sems.at[i])

    places_copy = begin(places_h, places, sems.at[1])
    local_copy = begin(local_h, local_rows, sems.at[0])
    if raw:
        send_copy = begin(edge_in_h.at[level, 1], w_send, sems.at[2])
    pre_copy(0).start()
    second = [
        begin(edge_out_h.at[level], w_out, sems.at[3]),
        begin(receivers_h, receivers, sems.at[4]),
        begin(gain_h, gain, sems.at[5]),
        begin(bias_h, bias, sems.at[6]),
    ]
    pre_copy(1).start()
    for i in range(blocks):
        edge_copy(i).start()
        if i + 2 < blocks:
            pre_copy(i + 2).start()
    third = [
        begin(nodes_h, nodes, sems.at[7]),
        begin(node_in_h.at[level], w_node, sems.at[8]),
        begin(node_out_h.at[level], w_node_out, sems.at[9]),
    ]
    if not last:
        third.append(begin(edge_in_h.at[level + 1, 1], w_next, sems.at[10]))
        third.append(begin(picks_h, picks, sems.at[11]))

    total[...] = jnp.zeros_like(total)
    start = local_rows.shape[0]
    for at in range(0, rows_in.shape[0], CHUNK):
        fill_table(table, start + at, rows_in[at:at + CHUNK, :].astype(F32) * 0.5)
    start += rows_in.shape[0]
    local_copy.wait()
    fill_table(table, 0, local_rows[...].astype(F32) * 0.5)
    if raw:
        send_copy.wait()
    for source in raw_rows:
        fill_table(table, start, project(source[...], w_send[...]).astype(F32) * 0.5)
        start += source.shape[0]
    places_copy.wait()

    def found(at):
        stage = stages[at // BLOCK % 2]
        base = at % BLOCK * tiles
        for j in range(8):
            stage[base + j * tiles:base + (j + 1) * tiles, :] = table[pl.ds(places[0, at + j], tiles), :]
        return [stage[pl.ds(base + tile, 8, stride=tiles), :] for tile in range(tiles)]

    def gather(i, group):
        halves = []
        for at in range(i * BLOCK + group * GROUP, i * BLOCK + (group + 1) * GROUP, 8):
            rows = found(at)
            halves.append([
                silu_of_half(pre[at:at + 8, t * LANES:(t + 1) * LANES] + rows[t]) for t in range(tiles)
            ])
        for t in range(tiles):
            both = jnp.concatenate([half[t] for half in halves], axis=0).astype(BF16)
            hidden[i % 2][group * GROUP:(group + 1) * GROUP, t * LANES:(t + 1) * LANES] = both

    def settle(i, group):
        rows = slice(i * BLOCK + group * GROUP, i * BLOCK + (group + 1) * GROUP)
        output = outputs[i % 2][group * GROUP:(group + 1) * GROUP, :]
        fresh = normalize(output, gain[level, 0:1, :], bias[level, 0:1, :])
        fresh_edges[rows, :] = (edges[rows, :].astype(F32) + fresh).astype(BF16)

    for turn in range(-2, blocks + 1):
        gathering = turn + 2 if turn + 2 < blocks else None
        multiplying = turn + 1 if 0 <= turn + 1 < blocks else None
        settling = turn if 0 <= turn < blocks else None
        adding = turn - 1 if turn >= 1 else None
        if gathering is not None:
            pre_copy(gathering).wait()
        if settling is not None:
            edge_copy(settling).wait()
        if turn == -1:
            for copy in second:
                copy.wait()
        if keep and adding is not None:
            fresh_copy(adding).start()
        if multiplying is not None:
            outputs[multiplying % 2][...] = dot(hidden[multiplying % 2][...], w_out[...])
        if adding is not None:
            rows = slice(adding * BLOCK, (adding + 1) * BLOCK)
            hot = hot_columns(receivers[:, rows], node_count).astype(BF16)
            total[...] += dot(hot, fresh_edges[rows, :])
        for group in range(BLOCK // GROUP):
            if gathering is not None:
                gather(gathering, group)
            if settling is not None:
                settle(settling, group)

    for copy in third:
        copy.wait()
    here = nodes[...]
    pre_node = dot(here, w_node[0]) + dot(total[...].astype(BF16), w_node[1])
    output = dot(silu_of_half(pre_node * 0.5).astype(BF16), w_node_out[...])
    updated = here.astype(F32) + normalize(output, gain[level, 1:2, :], bias[level, 1:2, :])
    updated = updated.astype(BF16)
    new_nodes[...] = updated
    ends = [begin(new_nodes, new_nodes_h, sems.at[12])]
    if not last:
        sent = project(updated, w_next[...])
        outgoing[...] = sent
        ends.append(begin(outgoing, outgoing_h, sems.at[13]))
        for i in range(out_rows.shape[0] // PICK_BLOCK):
            rows = pl.ds(i * PICK_BLOCK, PICK_BLOCK)
            out_rows[rows, :] = dot(picks[rows, :], sent).astype(BF16)
            ends.append(begin(out_rows.at[rows], out_rows_h.at[rows], pick_sems.at[i]))
    if keep:
        for i in range(blocks):
            fresh_copy(i).wait()
    for copy in ends:
        copy.wait()


HBM = pl.BlockSpec(memory_space=pltpu.HBM)
VMEM = pl.BlockSpec(memory_space=pltpu.VMEM)


def pinned(operands, specs):
    pin = pltpu.with_memory_space_constraint
    return [pin(operand, pltpu.HBM) if spec is HBM else operand for operand, spec in zip(operands, specs)]


def pre_stage(level, edges, receivers, nodes, edge_in, extra=(), shape=None):
    edge_count, width = edges.shape
    node_count = nodes.shape[0]
    blocks = edge_count // PRE_BLOCK
    operands = [edges, receivers, nodes, edge_in, *extra]
    out_shape = [pltpu.HBM((edge_count, width), F32)]
    line = pltpu.VMEM((1, edge_count), I32)
    weight = pltpu.VMEM((width, width), BF16)
    scratch = [
        pltpu.VMEM((edge_count, width), BF16), line, pltpu.VMEM((node_count, width), BF16),
        weight, weight, pltpu.VMEM((edge_count, width), F32),
    ]
    if shape:
        tile = extra[0]
        out_shape += [
            pltpu.HBM(tile.shape, BF16), pltpu.HBM((1, edge_count), I32), pltpu.HBM((1, edge_count), I32),
            pltpu.HBM((edge_count, node_count), BF16),
        ]
        tiled = pltpu.VMEM(tile.shape, BF16)
        scratch += [tiled, weight, line, line, tiled, line, line, line]
        scratch.append(pltpu.VMEM((edge_count, node_count), BF16))
    scratch += [pltpu.SemaphoreType.DMA((n,)) for n in (13, blocks, blocks)]
    in_specs = [HBM] * len(operands)
    return pl.pallas_call(
        functools.partial(pre_kernel, level, shape),
        out_shape=out_shape,
        in_specs=in_specs,
        out_specs=[HBM] * len(out_shape),
        scratch_shapes=scratch,
        name="pre_first" if shape else "pre_next",
        cost_estimate=pl.CostEstimate(
            flops=2 * edge_count * width * (width + node_count),
            bytes_accessed=edge_count * width * 6,
            transcendentals=0,
        ),
        compiler_params=pltpu.CompilerParams(vmem_limit_bytes=20 * MIB),
    )(*pinned(operands, in_specs))


def halo_stage(north, south, edge_in):
    rows, width = north.shape
    in_specs = [VMEM, VMEM, HBM]
    return pl.pallas_call(
        halo_kernel,
        out_shape=jax.ShapeDtypeStruct((2 * rows, width), BF16),
        in_specs=in_specs,
        out_specs=VMEM,
        scratch_shapes=[pltpu.VMEM((width, width), BF16), pltpu.SemaphoreType.DMA],
        name="halo_terms",
        cost_estimate=pl.CostEstimate(
            flops=4 * rows * width * width, bytes_accessed=6 * rows * width, transcendentals=0
        ),
        compiler_params=pltpu.CompilerParams(vmem_limit_bytes=8 * MIB),
    )(*pinned([north, south, edge_in], in_specs))


def main_stage(level, places, receivers, pre, edges, nodes, weights, tables, picks, last, keep):
    edge_count, width = edges.shape
    node_count = nodes.shape[0]
    operands = [places, receivers, pre, edges, nodes, *weights, *tables]
    in_specs = [HBM] * 12 + [VMEM] * (len(tables) - 1)
    out_shape = [pltpu.HBM((node_count, width), BF16)]
    blocks = edge_count // BLOCK
    table_rows = sum(piece.shape[0] for piece in tables)
    norm = pltpu.VMEM(weights[4].shape, F32)
    small = pltpu.VMEM((node_count, width), BF16)
    weight = pltpu.VMEM((width, width), BF16)
    scratch = [
        pltpu.VMEM((table_rows * (width // LANES), LANES), F32),
        pltpu.VMEM((BLOCK * (width // LANES), LANES), F32),
        pltpu.VMEM((BLOCK * (width // LANES), LANES), F32),
        pltpu.VMEM((BLOCK, width), BF16),
        pltpu.VMEM((BLOCK, width), BF16),
        pltpu.VMEM((BLOCK, width), F32),
        pltpu.VMEM((BLOCK, width), F32),
        pltpu.VMEM((node_count, width), F32),
        pltpu.SMEM((1, edge_count), I32),
        pltpu.VMEM((1, edge_count), I32),
        pltpu.VMEM((edge_count, width), F32),
        pltpu.VMEM((edge_count, width), BF16),
        small, weight, pltpu.VMEM((2, width, width), BF16), weight, norm, norm, small,
        pltpu.VMEM(tables[0].shape, BF16), pltpu.VMEM((edge_count, width), BF16),
    ]
    raw = len(tables) - 2
    if raw:
        scratch.append(weight)
    if not last:
        operands.append(picks)
        in_specs.append(HBM)
        rows = picks.shape[0]
        out_shape += [pltpu.HBM((node_count, width), BF16), pltpu.HBM((rows, width), BF16)]
        scratch += [weight, pltpu.VMEM(picks.shape, BF16), small, pltpu.VMEM((rows, width), BF16)]
    if keep:
        out_shape.append(pltpu.HBM((edge_count, width), BF16))
    scratch += [pltpu.SemaphoreType.DMA((n,)) for n in (14, blocks, blocks, blocks, edge_count // PICK_BLOCK)]
    return pl.pallas_call(
        functools.partial(main_kernel, level, raw, last, keep),
        out_shape=out_shape,
        in_specs=in_specs,
        out_specs=[HBM] * len(out_shape),
        scratch_shapes=scratch,
        name="encode" if level == 0 else "layer",
        cost_estimate=pl.CostEstimate(
            flops=2 * edge_count * width * (width + node_count),
            bytes_accessed=edge_count * width * 10,
            transcendentals=edge_count * width,
        ),
        compiler_params=pltpu.CompilerParams(vmem_limit_bytes=32 * MIB),
    )(*pinned(operands, in_specs))


def shift(array, axis, step, wrap):
    size = lax.axis_size(axis)
    pairs = [(i, (i + step) % size) for i in range(size) if wrap or 0 <= i + step < size]
    return lax.ppermute(array, axis, pairs)


def local(
    grid_latent,
    mesh_latent,
    g2m_edges,
    g2m_senders,
    g2m_receivers,
    mm_edges,
    mm_senders,
    mm_receivers,
    send_rows,
    edge_in,
    edge_out,
    node_in,
    node_out,
    norm_gain,
    norm_bias,
):
    high, wide, features = grid_latent.shape
    flat_tile = grid_latent.reshape(high * wide, features)
    weights = [edge_in, edge_out, node_in, node_out, norm_gain, norm_bias]

    north = shift(grid_latent, "lat", 1, False)
    south = shift(grid_latent, "lat", -1, False)
    pre, tile_terms, places, lines, picks = pre_stage(
        0, g2m_edges, g2m_receivers, mesh_latent, edge_in,
        (flat_tile, g2m_senders, mm_senders, send_rows), (high, wide),
    )
    north, south, tile_terms = lax.optimization_barrier((north, south, tile_terms))

    def column(first):
        pieces = [piece[:, first:first + HALO] for piece in (north, grid_latent, south)]
        return jnp.concatenate(pieces, axis=0).reshape(-1, features)

    west = shift(column(wide - HALO), "lon", 1, True)
    east = shift(column(0), "lon", -1, True)
    halo_terms = halo_stage(north.reshape(-1, features), south.reshape(-1, features), edge_in)
    tables = [tile_terms, halo_terms, west, east]
    nodes, outgoing, out_rows = main_stage(
        0, places, g2m_receivers, pre, g2m_edges, mesh_latent, weights, tables, picks, False, False
    )
    edges = mm_edges
    levels = edge_in.shape[0]
    devices = lax.axis_size("lat") * lax.axis_size("lon")
    for level in range(1, levels):
        blocks = out_rows.reshape(devices, -1, features)
        arrived = lax.all_to_all(blocks, ("lat", "lon"), split_axis=0, concat_axis=0, tiled=True)
        arrived = arrived.reshape(-1, features)
        (pre,) = pre_stage(level, edges, mm_receivers, nodes, edge_in)
        last = level == levels - 1
        results = main_stage(
            level, lines, mm_receivers, pre, edges, nodes, weights, [outgoing, arrived], picks,
            last, not last,
        )
        if last:
            (nodes,) = results
        else:
            nodes, outgoing, out_rows, edges = results
    return nodes


def solution(mesh):
    in_specs = (
        P("lat", "lon", None),
        P(("lat", "lon"), None),
        P(("lat", "lon"), None),
        P(("lat", "lon"), None),
        P(("lat", "lon"), None),
        P(("lat", "lon"), None),
        P(("lat", "lon"), None),
        P(("lat", "lon"), None),
        P(("lat", "lon"), None),
        P(),
        P(),
        P(),
        P(),
        P(),
        P(),
    )
    out_specs = P(("lat", "lon"), None)
    return jax.shard_map(local, mesh=mesh, in_specs=in_specs, out_specs=out_specs, check_vma=False)
```

```python
import functools

import jax
import jax.numpy as jnp
from jax import lax
from jax.experimental import pallas as pl
from jax.experimental.pallas import tpu as pltpu
from jax.sharding import PartitionSpec as P

HALO = 4
NORM_EPS = 1e-05
F32 = jnp.float32
BF16 = jnp.bfloat16
I32 = jnp.int32
BLOCK = 512
CHUNK = 256
GROUP = 32
PRE_BLOCK = 512
PICK_BLOCK = 256
LANES = 128
MIB = 1024 * 1024


def silu_of_half(half):
    return half + half * jnp.tanh(half)


def normalize(values, gains, biases):
    centre = jnp.mean(values, axis=-1, keepdims=True)
    shifted = values - centre
    spread = jnp.mean(shifted * shifted, axis=-1, keepdims=True)
    return shifted * lax.rsqrt(spread + NORM_EPS) * gains + biases


def dot(left, right):
    return jnp.dot(left, right, preferred_element_type=F32)


def project(values, weights):
    return dot(values, weights).astype(BF16)


def hot_columns(indices, nodes):
    places = lax.broadcasted_iota(I32, (nodes, indices.shape[1]), 0)
    return jnp.where(places == indices, 1.0, 0.0)


def hot_rows(indices, nodes):
    return hot_columns(indices, nodes).T.astype(BF16)


def cell_row(cell, high, wide):
    across = wide + 2 * HALO
    row = (cell * 241) >> 15
    column = cell - row * across
    band = jnp.where(row < HALO, 1, jnp.where(row < HALO + high, 0, 2))
    inner = row - jnp.where(band == 1, 0, jnp.where(band == 0, HALO, HALO + high))
    cells = high * wide
    tall = (high + 2 * HALO) * HALO
    side = 3 * cells + row * HALO
    west = side + column
    east = side + tall + column - HALO - wide
    centre = band * cells + inner * wide + column - HALO
    return jnp.where(column < HALO, west, jnp.where(column < HALO + wide, centre, east))


def begin(source, target, sem):
    copy = pltpu.make_async_copy(source, target, sem)
    copy.start()
    return copy


def part(ref, i, size=BLOCK):
    return ref.at[pl.ds(pl.multiple_of(i * size, size), size)]


def pre_kernel(level, shape, edges_h, receivers_h, nodes_h, edge_in_h, *refs):
    refs = list(refs)
    take = lambda count: [refs.pop(0) for _ in range(count)]
    if shape:
        tile_h, cells_h, senders_h, send_rows_h = take(4)
    pre_h = take(1)[0]
    if shape:
        tile_terms_h, places_h, lines_h, picks_h = take(4)
    edges, receivers, nodes, w_edge, w_recv, pre = take(6)
    if shape:
        tile, w_send, cells, senders, tile_terms, places, lines, send_rows, picks = take(9)
    sems, edge_sems, out_sems = take(3)
    node_count = nodes.shape[0]
    blocks = edges.shape[0] // PRE_BLOCK

    def edge_copy(i):
        return pltpu.make_async_copy(part(edges_h, i, PRE_BLOCK), part(edges, i, PRE_BLOCK), edge_sems.at[i])

    def out_copy(i):
        return pltpu.make_async_copy(part(pre, i, PRE_BLOCK), part(pre_h, i, PRE_BLOCK), out_sems.at[i])

    first = [
        begin(nodes_h, nodes, sems.at[0]),
        begin(edge_in_h.at[level, 2], w_recv, sems.at[1]),
        begin(receivers_h, receivers, sems.at[2]),
        begin(edge_in_h.at[level, 0], w_edge, sems.at[3]),
    ]
    edge_copy(0).start()
    if shape:
        second = [
            begin(tile_h, tile, sems.at[4]),
            begin(edge_in_h.at[level, 1], w_send, sems.at[5]),
            begin(cells_h, cells, sems.at[6]),
            begin(senders_h, senders, sems.at[7]),
            begin(send_rows_h, send_rows, sems.at[11]),
        ]
    for i in range(1, blocks):
        edge_copy(i).start()
    for copy in first:
        copy.wait()
    terms = project(nodes[...], w_recv[...])

    def step(i, _):
        rows = pl.ds(pl.multiple_of(i * PRE_BLOCK, PRE_BLOCK), PRE_BLOCK)
        edge_copy(i).wait()
        hot = hot_rows(jnp.minimum(receivers[:, rows], node_count - 1), node_count)
        pre[rows, :] = 0.5 * (dot(edges[rows, :], w_edge[...]) + dot(hot, terms))
        out_copy(i).start()
        return 0

    lax.fori_loop(0, blocks, step, 0)
    if shape:
        high, wide = shape
        tiles = edges.shape[1] // LANES
        for copy in second:
            copy.wait()

        def pick(i, _):
            rows = pl.ds(pl.multiple_of(i * PRE_BLOCK, PRE_BLOCK), PRE_BLOCK)
            picks[rows, :] = hot_rows(send_rows[:, rows], node_count)
            return 0

        lax.fori_loop(0, picks.shape[0] // PRE_BLOCK, pick, 0)
        tile_terms[...] = project(tile[...], w_send[...])
        ends = [begin(tile_terms, tile_terms_h, sems.at[8])]
        places[...] = cell_row(cells[...], high, wide) * tiles
        lines[...] = senders[...] * tiles
        ends.append(begin(places, places_h, sems.at[9]))
        ends.append(begin(lines, lines_h, sems.at[10]))
        ends.append(begin(picks, picks_h, sems.at[12]))
    for i in range(blocks):
        out_copy(i).wait()
    if shape:
        for copy in ends:
            copy.wait()


def halo_kernel(north, south, edge_in_h, terms, w_send, sem):
    begin(edge_in_h.at[0, 1], w_send, sem).wait()
    size = north.shape[0]
    terms[0:size, :] = project(north[...], w_send[...])
    terms[size:2 * size, :] = project(south[...], w_send[...])


def fill_table(table, start, values):
    tiles = values.shape[1] // LANES
    for group in range(values.shape[0] // 8):
        for tile in range(tiles):
            lines = pl.ds((start + group * 8) * tiles + tile, 8, stride=tiles)
            table[lines, :] = values[group * 8:group * 8 + 8, tile * LANES:(tile + 1) * LANES]


def main_kernel(level, raw, last, keep, *refs):
    refs = list(refs)
    take = lambda count: [refs.pop(0) for _ in range(count)]
    places_h, receivers_h, pre_h, edges_h, nodes_h = take(5)
    edge_in_h, edge_out_h, node_in_h, node_out_h, gain_h, bias_h = take(6)
    local_h, rows_in = take(2)
    raw_rows = take(raw)
    picks_h = None if last else take(1)[0]
    new_nodes_h = take(1)[0]
    outgoing_h, out_rows_h = (None, None) if last else take(2)
    new_edges_h = take(1)[0] if keep else None
    table, stage_0, stage_1, hidden_0, hidden_1, output_0, output_1 = take(7)
    total, places, receivers, pre, edges = take(5)
    nodes, w_out, w_node, w_node_out, gain, bias, new_nodes, local_rows, fresh_edges = take(9)
    w_send = take(1)[0] if raw else None
    w_next, picks, outgoing, out_rows = (None,) * 4 if last else take(4)
    sems, pre_sems, edge_sems, out_sems, pick_sems = take(5)

    node_count, width = nodes.shape
    blocks = edges.shape[0] // BLOCK
    tiles = width // LANES
    stages = [stage_0, stage_1]
    hidden = [hidden_0, hidden_1]
    outputs = [output_0, output_1]

    def pre_copy(i):
        return pltpu.make_async_copy(part(pre_h, i), part(pre, i), pre_sems.at[i])

    def edge_copy(i):
        return pltpu.make_async_copy(part(edges_h, i), part(edges, i), edge_sems.at[i])

    def fresh_copy(i):
        return pltpu.make_async_copy(part(fresh_edges, i), part(new_edges_h, i), out_sems.at[i])

    places_copy = begin(places_h, places, sems.at[1])
    local_copy = begin(local_h, local_rows, sems.at[0])
    if raw:
        send_copy = begin(edge_in_h.at[level, 1], w_send, sems.at[2])
    pre_copy(0).start()
    second = [
        begin(edge_out_h.at[level], w_out, sems.at[3]),
        begin(receivers_h, receivers, sems.at[4]),
        begin(gain_h, gain, sems.at[5]),
        begin(bias_h, bias, sems.at[6]),
    ]
    pre_copy(1).start()
    for i in range(blocks):
        edge_copy(i).start()
        if i + 2 < blocks:
            pre_copy(i + 2).start()
    third = [
        begin(nodes_h, nodes, sems.at[7]),
        begin(node_in_h.at[level], w_node, sems.at[8]),
        begin(node_out_h.at[level], w_node_out, sems.at[9]),
    ]
    if not last:
        third.append(begin(edge_in_h.at[level + 1, 1], w_next, sems.at[10]))
        third.append(begin(picks_h, picks, sems.at[11]))

    total[...] = jnp.zeros_like(total)
    start = local_rows.shape[0]
    for at in range(0, rows_in.shape[0], CHUNK):
        fill_table(table, start + at, rows_in[at:at + CHUNK, :].astype(F32) * 0.5)
    start += rows_in.shape[0]
    local_copy.wait()
    fill_table(table, 0, local_rows[...].astype(F32) * 0.5)
    if raw:
        send_copy.wait()
    for source in raw_rows:
        fill_table(table, start, project(source[...], w_send[...]).astype(F32) * 0.5)
        start += source.shape[0]
    places_copy.wait()

    def found(at):
        stage = stages[at // BLOCK % 2]
        base = at % BLOCK * tiles
        for j in range(8):
            stage[base + j * tiles:base + (j + 1) * tiles, :] = table[pl.ds(places[0, at + j], tiles), :]
        return [stage[pl.ds(base + tile, 8, stride=tiles), :] for tile in range(tiles)]

    def gather(i, group):
        halves = []
        for at in range(i * BLOCK + group * GROUP, i * BLOCK + (group + 1) * GROUP, 8):
            rows = found(at)
            halves.append([
                silu_of_half(pre[at:at + 8, t * LANES:(t + 1) * LANES] + rows[t]) for t in range(tiles)
            ])
        for t in range(tiles):
            both = jnp.concatenate([half[t] for half in halves], axis=0).astype(BF16)
            hidden[i % 2][group * GROUP:(group + 1) * GROUP, t * LANES:(t + 1) * LANES] = both

    def settle(i, group):
        rows = slice(i * BLOCK + group * GROUP, i * BLOCK + (group + 1) * GROUP)
        output = outputs[i % 2][group * GROUP:(group + 1) * GROUP, :]
        fresh = normalize(output, gain[level, 0:1, :], bias[level, 0:1, :])
        fresh_edges[rows, :] = (edges[rows, :].astype(F32) + fresh).astype(BF16)

    for turn in range(-2, blocks + 1):
        gathering = turn + 2 if turn + 2 < blocks else None
        multiplying = turn + 1 if 0 <= turn + 1 < blocks else None
        settling = turn if 0 <= turn < blocks else None
        adding = turn - 1 if turn >= 1 else None
        if gathering is not None:
            pre_copy(gathering).wait()
        if settling is not None:
            edge_copy(settling).wait()
        if turn == -1:
            for copy in second:
                copy.wait()
        if keep and adding is not None:
            fresh_copy(adding).start()
        if multiplying is not None:
            outputs[multiplying % 2][...] = dot(hidden[multiplying % 2][...], w_out[...])
        if adding is not None:
            rows = slice(adding * BLOCK, (adding + 1) * BLOCK)
            hot = hot_columns(receivers[:, rows], node_count).astype(BF16)
            total[...] += dot(hot, fresh_edges[rows, :])
        for group in range(BLOCK // GROUP):
            if gathering is not None:
                gather(gathering, group)
            if settling is not None:
                settle(settling, group)

    for copy in third:
        copy.wait()
    here = nodes[...]
    pre_node = dot(here, w_node[0]) + dot(total[...].astype(BF16), w_node[1])
    output = dot(silu_of_half(pre_node * 0.5).astype(BF16), w_node_out[...])
    updated = here.astype(F32) + normalize(output, gain[level, 1:2, :], bias[level, 1:2, :])
    updated = updated.astype(BF16)
    new_nodes[...] = updated
    ends = [begin(new_nodes, new_nodes_h, sems.at[12])]
    if not last:
        sent = project(updated, w_next[...])
        outgoing[...] = sent
        ends.append(begin(outgoing, outgoing_h, sems.at[13]))
        for i in range(out_rows.shape[0] // PICK_BLOCK):
            rows = pl.ds(i * PICK_BLOCK, PICK_BLOCK)
            out_rows[rows, :] = dot(picks[rows, :], sent).astype(BF16)
            ends.append(begin(out_rows.at[rows], out_rows_h.at[rows], pick_sems.at[i]))
    if keep:
        for i in range(blocks):
            fresh_copy(i).wait()
    for copy in ends:
        copy.wait()


HBM = pl.BlockSpec(memory_space=pltpu.HBM)
VMEM = pl.BlockSpec(memory_space=pltpu.VMEM)


def pinned(operands, specs):
    pin = pltpu.with_memory_space_constraint
    return [pin(operand, pltpu.HBM) if spec is HBM else operand for operand, spec in zip(operands, specs)]


def pre_stage(level, edges, receivers, nodes, edge_in, extra=(), shape=None):
    edge_count, width = edges.shape
    node_count = nodes.shape[0]
    blocks = edge_count // PRE_BLOCK
    operands = [edges, receivers, nodes, edge_in, *extra]
    out_shape = [pltpu.HBM((edge_count, width), F32)]
    line = pltpu.VMEM((1, edge_count), I32)
    weight = pltpu.VMEM((width, width), BF16)
    scratch = [
        pltpu.VMEM((edge_count, width), BF16), line, pltpu.VMEM((node_count, width), BF16),
        weight, weight, pltpu.VMEM((edge_count, width), F32),
    ]
    if shape:
        tile = extra[0]
        out_shape += [
            pltpu.HBM(tile.shape, BF16), pltpu.HBM((1, edge_count), I32), pltpu.HBM((1, edge_count), I32),
            pltpu.HBM((edge_count, node_count), BF16),
        ]
        tiled = pltpu.VMEM(tile.shape, BF16)
        scratch += [tiled, weight, line, line, tiled, line, line, line]
        scratch.append(pltpu.VMEM((edge_count, node_count), BF16))
    scratch += [pltpu.SemaphoreType.DMA((n,)) for n in (13, blocks, blocks)]
    in_specs = [HBM] * len(operands)
    return pl.pallas_call(
        functools.partial(pre_kernel, level, shape),
        out_shape=out_shape,
        in_specs=in_specs,
        out_specs=[HBM] * len(out_shape),
        scratch_shapes=scratch,
        name="pre_first" if shape else "pre_next",
        cost_estimate=pl.CostEstimate(
            flops=2 * edge_count * width * (width + node_count),
            bytes_accessed=edge_count * width * 6,
            transcendentals=0,
        ),
        compiler_params=pltpu.CompilerParams(vmem_limit_bytes=20 * MIB),
    )(*pinned(operands, in_specs))


def halo_stage(north, south, edge_in):
    rows, width = north.shape
    in_specs = [VMEM, VMEM, HBM]
    return pl.pallas_call(
        halo_kernel,
        out_shape=jax.ShapeDtypeStruct((2 * rows, width), BF16),
        in_specs=in_specs,
        out_specs=VMEM,
        scratch_shapes=[pltpu.VMEM((width, width), BF16), pltpu.SemaphoreType.DMA],
        name="halo_terms",
        cost_estimate=pl.CostEstimate(
            flops=4 * rows * width * width, bytes_accessed=6 * rows * width, transcendentals=0
        ),
        compiler_params=pltpu.CompilerParams(vmem_limit_bytes=8 * MIB),
    )(*pinned([north, south, edge_in], in_specs))


def main_stage(level, places, receivers, pre, edges, nodes, weights, tables, picks, last, keep):
    edge_count, width = edges.shape
    node_count = nodes.shape[0]
    operands = [places, receivers, pre, edges, nodes, *weights, *tables]
    in_specs = [HBM] * 12 + [VMEM] * (len(tables) - 1)
    out_shape = [pltpu.HBM((node_count, width), BF16)]
    blocks = edge_count // BLOCK
    table_rows = sum(piece.shape[0] for piece in tables)
    norm = pltpu.VMEM(weights[4].shape, F32)
    small = pltpu.VMEM((node_count, width), BF16)
    weight = pltpu.VMEM((width, width), BF16)
    scratch = [
        pltpu.VMEM((table_rows * (width // LANES), LANES), F32),
        pltpu.VMEM((BLOCK * (width // LANES), LANES), F32),
        pltpu.VMEM((BLOCK * (width // LANES), LANES), F32),
        pltpu.VMEM((BLOCK, width), BF16),
        pltpu.VMEM((BLOCK, width), BF16),
        pltpu.VMEM((BLOCK, width), F32),
        pltpu.VMEM((BLOCK, width), F32),
        pltpu.VMEM((node_count, width), F32),
        pltpu.SMEM((1, edge_count), I32),
        pltpu.VMEM((1, edge_count), I32),
        pltpu.VMEM((edge_count, width), F32),
        pltpu.VMEM((edge_count, width), BF16),
        small, weight, pltpu.VMEM((2, width, width), BF16), weight, norm, norm, small,
        pltpu.VMEM(tables[0].shape, BF16), pltpu.VMEM((edge_count, width), BF16),
    ]
    raw = len(tables) - 2
    if raw:
        scratch.append(weight)
    if not last:
        operands.append(picks)
        in_specs.append(HBM)
        rows = picks.shape[0]
        out_shape += [pltpu.HBM((node_count, width), BF16), pltpu.HBM((rows, width), BF16)]
        scratch += [weight, pltpu.VMEM(picks.shape, BF16), small, pltpu.VMEM((rows, width), BF16)]
    if keep:
        out_shape.append(pltpu.HBM((edge_count, width), BF16))
    scratch += [pltpu.SemaphoreType.DMA((n,)) for n in (14, blocks, blocks, blocks, edge_count // PICK_BLOCK)]
    return pl.pallas_call(
        functools.partial(main_kernel, level, raw, last, keep),
        out_shape=out_shape,
        in_specs=in_specs,
        out_specs=[HBM] * len(out_shape),
        scratch_shapes=scratch,
        name="encode" if level == 0 else "layer",
        cost_estimate=pl.CostEstimate(
            flops=2 * edge_count * width * (width + node_count),
            bytes_accessed=edge_count * width * 10,
            transcendentals=edge_count * width,
        ),
        compiler_params=pltpu.CompilerParams(vmem_limit_bytes=32 * MIB),
    )(*pinned(operands, in_specs))


def shift(array, axis, step, wrap):
    size = lax.axis_size(axis)
    pairs = [(i, (i + step) % size) for i in range(size) if wrap or 0 <= i + step < size]
    return lax.ppermute(array, axis, pairs)


def local(
    grid_latent,
    mesh_latent,
    g2m_edges,
    g2m_senders,
    g2m_receivers,
    mm_edges,
    mm_senders,
    mm_receivers,
    send_rows,
    edge_in,
    edge_out,
    node_in,
    node_out,
    norm_gain,
    norm_bias,
):
    high, wide, features = grid_latent.shape
    flat_tile = grid_latent.reshape(high * wide, features)
    weights = [edge_in, edge_out, node_in, node_out, norm_gain, norm_bias]

    lead = grid_latent[:, :HALO].reshape(-1, features)
    trail = grid_latent[:, wide - HALO:].reshape(-1, features)
    columns = jnp.concatenate([lead, trail], axis=0)
    north_columns = shift(columns, "lat", 1, False)
    south_columns = shift(columns, "lat", -1, False)
    north = shift(grid_latent, "lat", 1, False)
    south = shift(grid_latent, "lat", -1, False)
    middle = lead.shape[0]
    westward = jnp.concatenate([north_columns[:middle], lead, south_columns[:middle]], axis=0)
    eastward = jnp.concatenate([north_columns[middle:], trail, south_columns[middle:]], axis=0)
    westward, eastward, receivers = lax.optimization_barrier((westward, eastward, g2m_receivers))
    west = shift(eastward, "lon", 1, True)
    east = shift(westward, "lon", -1, True)
    pre, tile_terms, places, lines, picks = pre_stage(
        0, g2m_edges, receivers, mesh_latent, edge_in,
        (flat_tile, g2m_senders, mm_senders, send_rows), (high, wide),
    )
    north, south, tile_terms = lax.optimization_barrier((north, south, tile_terms))
    halo_terms = halo_stage(north.reshape(-1, features), south.reshape(-1, features), edge_in)
    tables = [tile_terms, halo_terms, west, east]
    nodes, outgoing, out_rows = main_stage(
        0, places, g2m_receivers, pre, g2m_edges, mesh_latent, weights, tables, picks, False, False
    )
    edges = mm_edges
    levels = edge_in.shape[0]
    devices = lax.axis_size("lat") * lax.axis_size("lon")
    for level in range(1, levels):
        blocks = out_rows.reshape(devices, -1, features)
        arrived = lax.all_to_all(blocks, ("lat", "lon"), split_axis=0, concat_axis=0, tiled=True)
        arrived = arrived.reshape(-1, features)
        (pre,) = pre_stage(level, edges, mm_receivers, nodes, edge_in)
        last = level == levels - 1
        results = main_stage(
            level, lines, mm_receivers, pre, edges, nodes, weights, [outgoing, arrived], picks,
            last, not last,
        )
        if last:
            (nodes,) = results
        else:
            nodes, outgoing, out_rows, edges = results
    return nodes


def solution(mesh):
    in_specs = (
        P("lat", "lon", None),
        P(("lat", "lon"), None),
        P(("lat", "lon"), None),
        P(("lat", "lon"), None),
        P(("lat", "lon"), None),
        P(("lat", "lon"), None),
        P(("lat", "lon"), None),
        P(("lat", "lon"), None),
        P(("lat", "lon"), None),
        P(),
        P(),
        P(),
        P(),
        P(),
        P(),
    )
    out_specs = P(("lat", "lon"), None)
    return jax.shard_map(local, mesh=mesh, in_specs=in_specs, out_specs=out_specs, check_vma=False)
```

```python
import functools

import jax
import jax.numpy as jnp
from jax import lax
from jax.experimental import pallas as pl
from jax.experimental.pallas import tpu as pltpu
from jax.sharding import PartitionSpec as P

HALO = 4
NORM_EPS = 1e-05
F32 = jnp.float32
BF16 = jnp.bfloat16
I32 = jnp.int32
SIZES = (256, 512, 512, 512, 256)
STARTS = tuple(sum(SIZES[:i]) for i in range(len(SIZES)))
BLOCK = max(SIZES)
CHUNK = 256
GROUP = 32
PRE_BLOCK = 512
PICK_BLOCK = 256
LANES = 128
MIB = 1024 * 1024


def silu_of_half(half):
    return half + half * jnp.tanh(half)


def normalize(values, gains, biases):
    centre = jnp.mean(values, axis=-1, keepdims=True)
    shifted = values - centre
    spread = jnp.mean(shifted * shifted, axis=-1, keepdims=True)
    return shifted * lax.rsqrt(spread + NORM_EPS) * gains + biases


def dot(left, right):
    return jnp.dot(left, right, preferred_element_type=F32)


def project(values, weights):
    return dot(values, weights).astype(BF16)


def hot_columns(indices, nodes):
    places = lax.broadcasted_iota(I32, (nodes, indices.shape[1]), 0)
    return jnp.where(places == indices, 1.0, 0.0)


def hot_rows(indices, nodes):
    return hot_columns(indices, nodes).T.astype(BF16)


def cell_row(cell, high, wide):
    across = wide + 2 * HALO
    row = (cell * 241) >> 15
    column = cell - row * across
    band = jnp.where(row < HALO, 1, jnp.where(row < HALO + high, 0, 2))
    inner = row - jnp.where(band == 1, 0, jnp.where(band == 0, HALO, HALO + high))
    cells = high * wide
    tall = (high + 2 * HALO) * HALO
    side = 3 * cells + row * HALO
    west = side + column
    east = side + tall + column - HALO - wide
    centre = band * cells + inner * wide + column - HALO
    return jnp.where(column < HALO, west, jnp.where(column < HALO + wide, centre, east))


def begin(source, target, sem):
    copy = pltpu.make_async_copy(source, target, sem)
    copy.start()
    return copy


def piece(ref, i):
    return ref.at[pl.ds(STARTS[i], SIZES[i])]


def part(ref, i, size):
    return ref.at[pl.ds(pl.multiple_of(i * size, size), size)]


def pre_kernel(level, shape, edges_h, receivers_h, nodes_h, edge_in_h, *refs):
    refs = list(refs)
    take = lambda count: [refs.pop(0) for _ in range(count)]
    if shape:
        tile_h, cells_h, senders_h, send_rows_h = take(4)
    pre_h = take(1)[0]
    if shape:
        tile_terms_h, places_h, lines_h, picks_h = take(4)
    edges, receivers, nodes, w_edge, w_recv, pre = take(6)
    if shape:
        tile, w_send, cells, senders, tile_terms, places, lines, send_rows, picks = take(9)
    sems, edge_sems, out_sems = take(3)
    node_count = nodes.shape[0]
    blocks = edges.shape[0] // PRE_BLOCK

    def edge_copy(i):
        return pltpu.make_async_copy(part(edges_h, i, PRE_BLOCK), part(edges, i, PRE_BLOCK), edge_sems.at[i])

    def out_copy(i):
        return pltpu.make_async_copy(part(pre, i, PRE_BLOCK), part(pre_h, i, PRE_BLOCK), out_sems.at[i])

    first = [
        begin(nodes_h, nodes, sems.at[0]),
        begin(edge_in_h.at[level, 2], w_recv, sems.at[1]),
        begin(receivers_h, receivers, sems.at[2]),
        begin(edge_in_h.at[level, 0], w_edge, sems.at[3]),
    ]
    edge_copy(0).start()
    if shape:
        second = [
            begin(tile_h, tile, sems.at[4]),
            begin(edge_in_h.at[level, 1], w_send, sems.at[5]),
            begin(cells_h, cells, sems.at[6]),
            begin(senders_h, senders, sems.at[7]),
            begin(send_rows_h, send_rows, sems.at[11]),
        ]
    for i in range(1, blocks):
        edge_copy(i).start()
    for copy in first:
        copy.wait()
    terms = project(nodes[...], w_recv[...])

    def step(i, _):
        rows = pl.ds(pl.multiple_of(i * PRE_BLOCK, PRE_BLOCK), PRE_BLOCK)
        edge_copy(i).wait()
        hot = hot_rows(jnp.minimum(receivers[:, rows], node_count - 1), node_count)
        pre[rows, :] = 0.5 * (dot(edges[rows, :], w_edge[...]) + dot(hot, terms))
        out_copy(i).start()
        return 0

    lax.fori_loop(0, blocks, step, 0)
    if shape:
        high, wide = shape
        tiles = edges.shape[1] // LANES
        for copy in second:
            copy.wait()

        def pick(i, _):
            rows = pl.ds(pl.multiple_of(i * PRE_BLOCK, PRE_BLOCK), PRE_BLOCK)
            picks[rows, :] = hot_rows(send_rows[:, rows], node_count)
            return 0

        lax.fori_loop(0, picks.shape[0] // PRE_BLOCK, pick, 0)
        tile_terms[...] = project(tile[...], w_send[...])
        ends = [begin(tile_terms, tile_terms_h, sems.at[8])]
        places[...] = cell_row(cells[...], high, wide) * tiles
        lines[...] = senders[...] * tiles
        ends.append(begin(places, places_h, sems.at[9]))
        ends.append(begin(lines, lines_h, sems.at[10]))
        ends.append(begin(picks, picks_h, sems.at[12]))
    for i in range(blocks):
        out_copy(i).wait()
    if shape:
        for copy in ends:
            copy.wait()


def halo_kernel(north, south, edge_in_h, terms, w_send, sem):
    begin(edge_in_h.at[0, 1], w_send, sem).wait()
    size = north.shape[0]
    terms[0:size, :] = project(north[...], w_send[...])
    terms[size:2 * size, :] = project(south[...], w_send[...])


def fill_table(table, start, values):
    tiles = values.shape[1] // LANES
    for group in range(values.shape[0] // 8):
        for tile in range(tiles):
            lines = pl.ds((start + group * 8) * tiles + tile, 8, stride=tiles)
            table[lines, :] = values[group * 8:group * 8 + 8, tile * LANES:(tile + 1) * LANES]


def main_kernel(level, raw, last, keep, *refs):
    refs = list(refs)
    take = lambda count: [refs.pop(0) for _ in range(count)]
    places_h, receivers_h, pre_h, edges_h, nodes_h = take(5)
    edge_in_h, edge_out_h, node_in_h, node_out_h, gain_h, bias_h = take(6)
    local_h, rows_in = take(2)
    raw_rows = take(raw)
    picks_h = None if last else take(1)[0]
    new_nodes_h = take(1)[0]
    outgoing_h, out_rows_h = (None, None) if last else take(2)
    new_edges_h = take(1)[0] if keep else None
    table, stage_0, stage_1, hidden_0, hidden_1, output_0, output_1 = take(7)
    total, places, receivers, pre, edges = take(5)
    nodes, w_out, w_node, w_node_out, gain, bias, new_nodes, local_rows, fresh_edges = take(9)
    w_send = take(1)[0] if raw else None
    w_next, picks, outgoing, out_rows = (None,) * 4 if last else take(4)
    sems, pre_sems, edge_sems, out_sems, pick_sems = take(5)

    node_count, width = nodes.shape
    blocks = len(SIZES)
    tiles = width // LANES
    stages = [stage_0, stage_1]
    hidden = [hidden_0, hidden_1]
    outputs = [output_0, output_1]

    def pre_copy(i):
        return pltpu.make_async_copy(piece(pre_h, i), piece(pre, i), pre_sems.at[i])

    def edge_copy(i):
        return pltpu.make_async_copy(piece(edges_h, i), piece(edges, i), edge_sems.at[i])

    def fresh_copy(i):
        return pltpu.make_async_copy(piece(fresh_edges, i), piece(new_edges_h, i), out_sems.at[i])

    places_copy = begin(places_h, places, sems.at[1])
    local_copy = begin(local_h, local_rows, sems.at[0])
    if raw:
        send_copy = begin(edge_in_h.at[level, 1], w_send, sems.at[2])
    pre_copy(0).start()
    second = [
        begin(edge_out_h.at[level], w_out, sems.at[3]),
        begin(receivers_h, receivers, sems.at[4]),
        begin(gain_h, gain, sems.at[5]),
        begin(bias_h, bias, sems.at[6]),
    ]
    pre_copy(1).start()
    for i in range(blocks):
        edge_copy(i).start()
        if i + 2 < blocks:
            pre_copy(i + 2).start()
    third = [
        begin(nodes_h, nodes, sems.at[7]),
        begin(node_in_h.at[level], w_node, sems.at[8]),
        begin(node_out_h.at[level], w_node_out, sems.at[9]),
    ]
    if not last:
        third.append(begin(edge_in_h.at[level + 1, 1], w_next, sems.at[10]))
        third.append(begin(picks_h, picks, sems.at[11]))

    total[...] = jnp.zeros_like(total)
    start = local_rows.shape[0]
    for at in range(0, rows_in.shape[0], CHUNK):
        fill_table(table, start + at, rows_in[at:at + CHUNK, :].astype(F32) * 0.5)
    start += rows_in.shape[0]
    local_copy.wait()
    fill_table(table, 0, local_rows[...].astype(F32) * 0.5)
    if raw:
        send_copy.wait()
    for source in raw_rows:
        fill_table(table, start, project(source[...], w_send[...]).astype(F32) * 0.5)
        start += source.shape[0]
    places_copy.wait()

    def found(i, at):
        stage = stages[i % 2]
        base = (at - STARTS[i]) * tiles
        for j in range(8):
            stage[base + j * tiles:base + (j + 1) * tiles, :] = table[pl.ds(places[0, at + j], tiles), :]
        return [stage[pl.ds(base + tile, 8, stride=tiles), :] for tile in range(tiles)]

    def gather(i, group):
        halves = []
        first = STARTS[i] + group * GROUP
        for at in range(first, first + GROUP, 8):
            rows = found(i, at)
            halves.append([
                silu_of_half(pre[at:at + 8, t * LANES:(t + 1) * LANES] + rows[t]) for t in range(tiles)
            ])
        for t in range(tiles):
            both = jnp.concatenate([half[t] for half in halves], axis=0).astype(BF16)
            hidden[i % 2][group * GROUP:(group + 1) * GROUP, t * LANES:(t + 1) * LANES] = both

    def settle(i, group):
        rows = slice(STARTS[i] + group * GROUP, STARTS[i] + (group + 1) * GROUP)
        output = outputs[i % 2][group * GROUP:(group + 1) * GROUP, :]
        fresh = normalize(output, gain[level, 0:1, :], bias[level, 0:1, :])
        fresh_edges[rows, :] = (edges[rows, :].astype(F32) + fresh).astype(BF16)

    for turn in range(-2, blocks + 1):
        gathering = turn + 2 if turn + 2 < blocks else None
        multiplying = turn + 1 if 0 <= turn + 1 < blocks else None
        settling = turn if 0 <= turn < blocks else None
        adding = turn - 1 if turn >= 1 else None
        if gathering is not None:
            pre_copy(gathering).wait()
        if settling is not None:
            edge_copy(settling).wait()
        if turn == -1:
            for copy in second:
                copy.wait()
        if keep and adding is not None:
            fresh_copy(adding).start()
        if multiplying is not None:
            size = SIZES[multiplying]
            outputs[multiplying % 2][0:size, :] = dot(hidden[multiplying % 2][0:size, :], w_out[...])
        if adding is not None:
            rows = slice(STARTS[adding], STARTS[adding] + SIZES[adding])
            hot = hot_columns(receivers[:, rows], node_count).astype(BF16)
            total[...] += dot(hot, fresh_edges[rows, :])
        for group in range(BLOCK // GROUP):
            if gathering is not None and group < SIZES[gathering] // GROUP:
                gather(gathering, group)
            if settling is not None and group < SIZES[settling] // GROUP:
                settle(settling, group)

    for copy in third:
        copy.wait()
    here = nodes[...]
    pre_node = dot(here, w_node[0]) + dot(total[...].astype(BF16), w_node[1])
    output = dot(silu_of_half(pre_node * 0.5).astype(BF16), w_node_out[...])
    updated = here.astype(F32) + normalize(output, gain[level, 1:2, :], bias[level, 1:2, :])
    updated = updated.astype(BF16)
    new_nodes[...] = updated
    ends = [begin(new_nodes, new_nodes_h, sems.at[12])]
    if not last:
        sent = project(updated, w_next[...])
        outgoing[...] = sent
        ends.append(begin(outgoing, outgoing_h, sems.at[13]))
        for i in range(out_rows.shape[0] // PICK_BLOCK):
            rows = pl.ds(i * PICK_BLOCK, PICK_BLOCK)
            out_rows[rows, :] = dot(picks[rows, :], sent).astype(BF16)
            ends.append(begin(out_rows.at[rows], out_rows_h.at[rows], pick_sems.at[i]))
    if keep:
        for i in range(blocks):
            fresh_copy(i).wait()
    for copy in ends:
        copy.wait()


HBM = pl.BlockSpec(memory_space=pltpu.HBM)
VMEM = pl.BlockSpec(memory_space=pltpu.VMEM)


def pinned(operands, specs):
    pin = pltpu.with_memory_space_constraint
    return [pin(operand, pltpu.HBM) if spec is HBM else operand for operand, spec in zip(operands, specs)]


def pre_stage(level, edges, receivers, nodes, edge_in, extra=(), shape=None):
    edge_count, width = edges.shape
    node_count = nodes.shape[0]
    blocks = edge_count // PRE_BLOCK
    operands = [edges, receivers, nodes, edge_in, *extra]
    out_shape = [pltpu.HBM((edge_count, width), F32)]
    line = pltpu.VMEM((1, edge_count), I32)
    weight = pltpu.VMEM((width, width), BF16)
    scratch = [
        pltpu.VMEM((edge_count, width), BF16), line, pltpu.VMEM((node_count, width), BF16),
        weight, weight, pltpu.VMEM((edge_count, width), F32),
    ]
    if shape:
        tile = extra[0]
        out_shape += [
            pltpu.HBM(tile.shape, BF16), pltpu.HBM((1, edge_count), I32), pltpu.HBM((1, edge_count), I32),
            pltpu.HBM((edge_count, node_count), BF16),
        ]
        tiled = pltpu.VMEM(tile.shape, BF16)
        scratch += [tiled, weight, line, line, tiled, line, line, line]
        scratch.append(pltpu.VMEM((edge_count, node_count), BF16))
    scratch += [pltpu.SemaphoreType.DMA((n,)) for n in (13, blocks, blocks)]
    in_specs = [HBM] * len(operands)
    return pl.pallas_call(
        functools.partial(pre_kernel, level, shape),
        out_shape=out_shape,
        in_specs=in_specs,
        out_specs=[HBM] * len(out_shape),
        scratch_shapes=scratch,
        name="pre_first" if shape else "pre_next",
        cost_estimate=pl.CostEstimate(
            flops=2 * edge_count * width * (width + node_count),
            bytes_accessed=edge_count * width * 6,
            transcendentals=0,
        ),
        compiler_params=pltpu.CompilerParams(vmem_limit_bytes=20 * MIB),
    )(*pinned(operands, in_specs))


def halo_stage(north, south, edge_in):
    rows, width = north.shape
    in_specs = [VMEM, VMEM, HBM]
    return pl.pallas_call(
        halo_kernel,
        out_shape=jax.ShapeDtypeStruct((2 * rows, width), BF16),
        in_specs=in_specs,
        out_specs=VMEM,
        scratch_shapes=[pltpu.VMEM((width, width), BF16), pltpu.SemaphoreType.DMA],
        name="halo_terms",
        cost_estimate=pl.CostEstimate(
            flops=4 * rows * width * width, bytes_accessed=6 * rows * width, transcendentals=0
        ),
        compiler_params=pltpu.CompilerParams(vmem_limit_bytes=8 * MIB),
    )(*pinned([north, south, edge_in], in_specs))


def main_stage(level, places, receivers, pre, edges, nodes, weights, tables, picks, last, keep):
    edge_count, width = edges.shape
    node_count = nodes.shape[0]
    operands = [places, receivers, pre, edges, nodes, *weights, *tables]
    in_specs = [HBM] * 12 + [VMEM] * (len(tables) - 1)
    out_shape = [pltpu.HBM((node_count, width), BF16)]
    blocks = len(SIZES)
    table_rows = sum(piece.shape[0] for piece in tables)
    norm = pltpu.VMEM(weights[4].shape, F32)
    small = pltpu.VMEM((node_count, width), BF16)
    weight = pltpu.VMEM((width, width), BF16)
    scratch = [
        pltpu.VMEM((table_rows * (width // LANES), LANES), F32),
        pltpu.VMEM((BLOCK * (width // LANES), LANES), F32),
        pltpu.VMEM((BLOCK * (width // LANES), LANES), F32),
        pltpu.VMEM((BLOCK, width), BF16),
        pltpu.VMEM((BLOCK, width), BF16),
        pltpu.VMEM((BLOCK, width), F32),
        pltpu.VMEM((BLOCK, width), F32),
        pltpu.VMEM((node_count, width), F32),
        pltpu.SMEM((1, edge_count), I32),
        pltpu.VMEM((1, edge_count), I32),
        pltpu.VMEM((edge_count, width), F32),
        pltpu.VMEM((edge_count, width), BF16),
        small, weight, pltpu.VMEM((2, width, width), BF16), weight, norm, norm, small,
        pltpu.VMEM(tables[0].shape, BF16), pltpu.VMEM((edge_count, width), BF16),
    ]
    raw = len(tables) - 2
    if raw:
        scratch.append(weight)
    if not last:
        operands.append(picks)
        in_specs.append(HBM)
        rows = picks.shape[0]
        out_shape += [pltpu.HBM((node_count, width), BF16), pltpu.HBM((rows, width), BF16)]
        scratch += [weight, pltpu.VMEM(picks.shape, BF16), small, pltpu.VMEM((rows, width), BF16)]
    if keep:
        out_shape.append(pltpu.HBM((edge_count, width), BF16))
    scratch += [pltpu.SemaphoreType.DMA((n,)) for n in (14, blocks, blocks, blocks, edge_count // PICK_BLOCK)]
    return pl.pallas_call(
        functools.partial(main_kernel, level, raw, last, keep),
        out_shape=out_shape,
        in_specs=in_specs,
        out_specs=[HBM] * len(out_shape),
        scratch_shapes=scratch,
        name="encode" if level == 0 else "layer",
        cost_estimate=pl.CostEstimate(
            flops=2 * edge_count * width * (width + node_count),
            bytes_accessed=edge_count * width * 10,
            transcendentals=edge_count * width,
        ),
        compiler_params=pltpu.CompilerParams(vmem_limit_bytes=32 * MIB),
    )(*pinned(operands, in_specs))


def shift(array, axis, step, wrap):
    size = lax.axis_size(axis)
    pairs = [(i, (i + step) % size) for i in range(size) if wrap or 0 <= i + step < size]
    return lax.ppermute(array, axis, pairs)


def local(
    grid_latent,
    mesh_latent,
    g2m_edges,
    g2m_senders,
    g2m_receivers,
    mm_edges,
    mm_senders,
    mm_receivers,
    send_rows,
    edge_in,
    edge_out,
    node_in,
    node_out,
    norm_gain,
    norm_bias,
):
    high, wide, features = grid_latent.shape
    flat_tile = grid_latent.reshape(high * wide, features)
    weights = [edge_in, edge_out, node_in, node_out, norm_gain, norm_bias]

    north = shift(grid_latent, "lat", 1, False)
    south = shift(grid_latent, "lat", -1, False)
    pre, tile_terms, places, lines, picks = pre_stage(
        0, g2m_edges, g2m_receivers, mesh_latent, edge_in,
        (flat_tile, g2m_senders, mm_senders, send_rows), (high, wide),
    )
    north, south, tile_terms = lax.optimization_barrier((north, south, tile_terms))

    def column(first):
        pieces = [piece[:, first:first + HALO] for piece in (north, grid_latent, south)]
        return jnp.concatenate(pieces, axis=0).reshape(-1, features)

    west = shift(column(wide - HALO), "lon", 1, True)
    east = shift(column(0), "lon", -1, True)
    halo_terms = halo_stage(north.reshape(-1, features), south.reshape(-1, features), edge_in)
    tables = [tile_terms, halo_terms, west, east]
    nodes, outgoing, out_rows = main_stage(
        0, places, g2m_receivers, pre, g2m_edges, mesh_latent, weights, tables, picks, False, False
    )
    edges = mm_edges
    levels = edge_in.shape[0]
    devices = lax.axis_size("lat") * lax.axis_size("lon")
    for level in range(1, levels):
        blocks = out_rows.reshape(devices, -1, features)
        arrived = lax.all_to_all(blocks, ("lat", "lon"), split_axis=0, concat_axis=0, tiled=True)
        arrived = arrived.reshape(-1, features)
        (pre,) = pre_stage(level, edges, mm_receivers, nodes, edge_in)
        last = level == levels - 1
        results = main_stage(
            level, lines, mm_receivers, pre, edges, nodes, weights, [outgoing, arrived], picks,
            last, not last,
        )
        if last:
            (nodes,) = results
        else:
            nodes, outgoing, out_rows, edges = results
    return nodes


def solution(mesh):
    in_specs = (
        P("lat", "lon", None),
        P(("lat", "lon"), None),
        P(("lat", "lon"), None),
        P(("lat", "lon"), None),
        P(("lat", "lon"), None),
        P(("lat", "lon"), None),
        P(("lat", "lon"), None),
        P(("lat", "lon"), None),
        P(("lat", "lon"), None),
        P(),
        P(),
        P(),
        P(),
        P(),
        P(),
    )
    out_specs = P(("lat", "lon"), None)
    return jax.shard_map(local, mesh=mesh, in_specs=in_specs, out_specs=out_specs, check_vma=False)
```
